256 devices in a mesh: trial: 2 (over z_hi), shard: 32 (over y, x, core), cols: 4 (over z_lo).
Axes of the slice: x: 4, y: 4, z: 8 (z_hi: 2, z_lo: 4; z = z_hi * 4 + z_lo), core: 2. Of those that a mesh axis runs over, the one named last changes fastest.
Arguments:
- train_gate: bfloat16 [4096, 8192], P(('trial', 'shard'), 'cols'), parts along dimension 0, may hold values from -0.125 to 0.125
- low_gate: bfloat16 [4096, 16], P(('trial', 'shard')), parts along dimension 0, may hold values from -0.125 to 0.125
- high_gate: bfloat16 [32, 8192], P('trial', 'cols'), parts along dimension 0, may hold values from -1.5 to 1.5
- train_up: bfloat16 [4096, 8192], P(('trial', 'shard'), 'cols'), parts along dimension 0, may hold values from -0.125 to 0.125
- low_up: bfloat16 [4096, 16], P(('trial', 'shard')), parts along dimension 0, may hold values from -0.125 to 0.125
- high_up: bfloat16 [32, 8192], P('trial', 'cols'), parts along dimension 0, may hold values from -1.5 to 1.5
- norm_train: float32 [4096], P(('trial', 'shard', 'cols')), parts along dimension 0, may hold values from 0.25 to 1.75
- norm_step: float32 [4096], P(('trial', 'shard', 'cols')), parts along dimension 0, may hold values from -0.3 to 0.3
Outputs:
- serve_gate: bfloat16 [16384, 2048], P(('trial', 'cols')), parts along dimension 0
- serve_up: bfloat16 [16384, 2048], P(('trial', 'cols')), parts along dimension 0
- serve_norm: bfloat16 [4096], P('trial'), parts along dimension 0
The draws below stay inside these ranges and needn't reach their ends.
There are 2 independent parts, one for each index of `trial`. The reference program is written for one: setup_inputs(seed, part) draws one part's arguments, and reference() takes and returns one part's arrays. A program takes and returns all parts, laid end to end along the dimension named above; each array names one. Nothing has to cross between parts.
All inputs are finite; a program needn't handle non-finite values.
Results may differ from the reference program's by a relative error of at most 0.001.
Values may be sent and summed in bfloat16 or wider, within the bound.
A program may use at most 128 MiB of HBM per device.

```python
import jax
import jax.numpy as jnp

D_MODEL = 2048
D_INNER = 8192
RANK = 16


def steps_of(stream_key, extent, shards, low, largest):
    gain = 1.0
    for position, blocks in shards:
        heights = jax.random.uniform(jax.random.fold_in(jax.random.fold_in(stream_key, 6), position), (blocks,), jnp.float32, low / len(shards), largest / len(shards))
        gain = gain * jnp.repeat(jnp.exp(heights), extent[position] // blocks).reshape((-1,) + (1,) * (len(extent) - 1 - position))
    return gain


def centred(key, shape, width, reach, cuts=(), kind=jnp.bfloat16):
    loudness = steps_of(key, shape, cuts, -0.22, 0.18) if cuts else 1.0
    array = jax.random.normal(key, shape, jnp.float32) * width * loudness
    return jnp.minimum(jnp.maximum(array, -reach), reach).astype(kind)


def setup_inputs(seed: int = 0, part: int = 0) -> dict:
    key_list = jax.random.split(jax.random.key(seed), 9)
    part_splits = jax.random.split(jax.random.fold_in(key_list[8], part), 9)
    return {
        "train_gate": centred(part_splits[0], (D_MODEL, D_INNER), D_MODEL ** -0.5, 0.125, ((0, 32), (1, 4))),
        "low_gate": centred(part_splits[1], (D_MODEL, RANK), D_MODEL ** -0.5, 0.125, ((0, 32),)),
        "high_gate": centred(part_splits[2], (RANK, D_INNER), RANK ** -0.5, 1.5, ((1, 4),)),
        "train_up": centred(part_splits[3], (D_MODEL, D_INNER), D_MODEL ** -0.5, 0.125, ((0, 32), (1, 4))),
        "low_up": centred(part_splits[4], (D_MODEL, RANK), D_MODEL ** -0.5, 0.125, ((0, 32),)),
        "high_up": centred(part_splits[5], (RANK, D_INNER), RANK ** -0.5, 1.5, ((1, 4),)),
        "norm_train": jnp.clip(1.0 + 0.15 * jax.random.normal(part_splits[6], (D_MODEL,), jnp.float32), 0.25, 1.75),
        "norm_step": jnp.clip(jax.random.uniform(part_splits[7], (D_MODEL,), jnp.float32, -0.3, 0.3) * steps_of(part_splits[7], (D_MODEL,), ((0, 128),), -0.4, 0.0), -0.3, 0.3),
    }


mix_rate = 2.0


def reference(train_gate, low_gate, high_gate, train_up, low_up, high_up, norm_train, norm_step):
    fresh_gate = train_gate.astype(jnp.float32) + mix_rate * jnp.dot(low_gate, high_gate, preferred_element_type=jnp.float32)
    fresh_up = train_up.astype(jnp.float32) + mix_rate * jnp.dot(low_up, high_up, preferred_element_type=jnp.float32)
    serve_gate = fresh_gate.T.astype(jnp.bfloat16)
    serve_up = fresh_up.T.astype(jnp.bfloat16)
    serve_norm = (norm_train + norm_step).astype(jnp.bfloat16)
    return serve_gate, serve_up, serve_norm
```

```python
import functools

import jax
import jax.numpy as jnp
from jax import lax
from jax.experimental import pallas as pl
from jax.experimental.pallas import tpu as pltpu
from jax.sharding import Mesh
from jax.sharding import PartitionSpec as P

TRIAL_SHARD = ("trial", "y", "x", "core")
TRIAL_SHARD_COLS = ("trial", "y", "x", "core", "cols")
MESH_ID = pl.DeviceIdType.MESH
MIX_RATE = 2.0
SIDE = 4
CHIPS = SIDE * SIDE
LANES = 128


def fresh(train, low, high):
    return train[...].astype(jnp.float32) + MIX_RATE * jnp.dot(
        low[...], high[...], preferred_element_type=jnp.float32
    )


def gather_kernel(
    train_gate, low_gate, high_gate, train_up, low_up, high_up, norm_train, norm_step,
    gate, up, norm,
    gate_sent, gate_came, gate_gave, gate_got, up_sent, up_came, up_gave, up_got, norm_sent, norm_came,
):
    y, x, core, col = (lax.axis_index(a) for a in ("y", "x", "core", "cols"))
    sibling = 1 - core

    def wrap(i):
        return lax.rem(i + SIDE, SIDE)

    neighbours = [{"x": wrap(x + 1)}, {"x": wrap(x - 1)}, {"y": wrap(y + 1)}, {"y": wrap(y - 1)}]
    partners = [{"core": sibling}] + [{"cols": wrap(col + k)} for k in (1, 2, 3)]

    barrier = pltpu.get_barrier_semaphore()
    for device in neighbours + partners:
        pl.semaphore_signal(barrier, inc=1, device_id=device, device_id_type=MESH_ID)

    mine = y * SIDE + x
    gate[core, mine] = fresh(train_gate, low_gate, high_gate).astype(jnp.bfloat16)
    up[core, mine] = fresh(train_up, low_up, high_up).astype(jnp.bfloat16)
    lane = lax.broadcasted_iota(jnp.int32, (1, LANES), 1)
    row = jnp.zeros((1, LANES), jnp.float32)
    first = core * 64 + col * 16
    for i in range(16):
        row = jnp.where(lane == first + i, norm_train[i] + norm_step[i], row)
    norm[core, y, x, col] = row

    pl.semaphore_wait(barrier, len(neighbours + partners))

    def send(src, dst, sent, came, device):
        pltpu.make_async_remote_copy(
            src_ref=src, dst_ref=dst, send_sem=sent, recv_sem=came, device_id=device, device_id_type=MESH_ID
        ).start()

    def arrive(ref, sem):
        pltpu.make_async_copy(ref, ref, sem).wait()

    class Stream:
        def __init__(self, fast_is_x, ref, sent, came, gave, got):
            self.fast_is_x, self.ref = fast_is_x, ref
            self.sent, self.came, self.gave, self.took = sent, came, gave, got

        def chip(self, f, s):
            f, s = (wrap(f + x), wrap(s + y)) if self.fast_is_x else (wrap(f + y), wrap(s + x))
            return s * SIDE + f if self.fast_is_x else f * SIDE + s

        def device(self, along_fast, step):
            axis, at = ("x", x) if along_fast == self.fast_is_x else ("y", y)
            return {axis: wrap(at + step)}

        def block(self, f, s, half=None):
            rows = slice(None) if half is None else pl.ds(half * 32, 32)
            return self.ref.at[core, self.chip(f, s), rows]

        def push(self, along_fast, step, f, s, half, slot):
            piece = self.block(f, s, half)
            send(piece, piece, self.sent, self.came.at[slot], self.device(along_fast, step))

        def share(self, piece):
            send(piece, piece, self.gave, self.took, {"core": sibling})

        def got(self, f, s, half, slot):
            piece = self.block(f, s, half)
            arrive(piece, self.came.at[slot])
            self.share(piece)

    a = Stream(True, gate, gate_sent, gate_came, gate_gave, gate_got)
    b = Stream(False, up, up_sent, up_came, up_gave, up_got)
    both = (a, b)

    def fast_own(st):
        st.push(True, 1, 0, 0, None, 0)
        st.push(True, -1, 0, 0, None, 1)

    def fast_near(st):
        st.got(-1, 0, None, 0)
        st.push(True, 1, -1, 0, 0, 2)
        st.got(1, 0, None, 1)
        st.push(True, -1, 1, 0, 1, 3)

    def fast_far(st):
        st.got(2, 0, 0, 2)
        st.got(2, 0, 1, 3)

    def slow_own(st, f):
        k = 4 + 4 * (f % 4)
        st.push(False, 1, f, 0, None, k)
        st.push(False, -1, f, 0, None, k + 1)

    def slow_near(st, f):
        k = 4 + 4 * (f % 4)
        st.got(f, -1, None, k)
        st.push(False, 1, f, -1, 0, k + 2)
        st.got(f, 1, None, k + 1)
        st.push(False, -1, f, 1, 1, k + 3)

    def slow_far(st, f):
        k = 4 + 4 * (f % 4)
        st.got(f, 2, 0, k + 2)
        st.got(f, 2, 1, k + 3)

    own_norm = norm.at[core, y, x, col]
    for k in (1, 2, 3):
        send(own_norm, own_norm, norm_sent.at[k - 1], norm_came.at[k - 1], {"cols": wrap(col + k)})
    for st in both:
        fast_own(st)
    for st in both:
        slow_own(st, 0)
    for st in both:
        st.share(st.block(0, 0))

    for k in (1, 2, 3):
        arrive(norm.at[core, y, x, wrap(col - k)], norm_came.at[k - 1])
    own_norm = norm.at[core, y, x]
    send(own_norm, own_norm, norm_sent.at[3], norm_came.at[3], {"x": wrap(x + 1)})
    send(own_norm, own_norm, norm_sent.at[4], norm_came.at[4], {"x": wrap(x - 1)})

    for st in both:
        fast_near(st)
    arrive(norm.at[core, y, wrap(x - 1)], norm_came.at[3])
    arrive(norm.at[core, y, wrap(x + 1)], norm_came.at[4])
    far_norm = norm.at[core, y, wrap(x - 1)]
    send(far_norm, far_norm, norm_sent.at[5], norm_came.at[5], {"x": wrap(x + 1)})
    for f in (-1, 1):
        for st in both:
            slow_own(st, f)
    for st in both:
        slow_near(st, 0)
    arrive(norm.at[core, y, wrap(x + 2)], norm_came.at[5])
    norm_rows = norm.at[core, y]
    send(norm_rows, norm_rows, norm_sent.at[6], norm_came.at[6], {"y": wrap(y + 1)})
    send(norm_rows, norm_rows, norm_sent.at[7], norm_came.at[7], {"y": wrap(y - 1)})
    for st in both:
        fast_far(st)
    for st in both:
        slow_own(st, 2)
    for f in (-1, 1):
        for st in both:
            slow_near(st, f)
    arrive(norm.at[core, wrap(y - 1)], norm_came.at[6])
    arrive(norm.at[core, wrap(y + 1)], norm_came.at[7])
    far_rows = norm.at[core, wrap(y - 1)]
    send(far_rows, far_rows, norm_sent.at[8], norm_came.at[8], {"y": wrap(y + 1)})
    for st in both:
        slow_far(st, 0)
    for f in (-1, 1):
        for st in both:
            slow_far(st, f)
    arrive(norm.at[core, wrap(y + 2)], norm_came.at[8])
    send(norm.at[core], norm.at[core], norm_sent.at[9], norm_came.at[9], {"core": sibling})
    for st in both:
        slow_near(st, 2)
    for st in both:
        slow_far(st, 2)

    for st in both:
        arrive(st.ref.at[core, pl.ds(0, 15)], st.sent)
        arrive(st.ref.at[core], st.gave)
        arrive(st.ref.at[sibling], st.took)
    for k in range(3):
        arrive(norm.at[core, y, x, col], norm_sent.at[k])
    for k in range(3, 6):
        arrive(norm.at[core, y, x], norm_sent.at[k])
    for k in range(6, 9):
        arrive(norm.at[core, y], norm_sent.at[k])
    arrive(norm.at[core], norm_sent.at[9])
    arrive(norm.at[sibling], norm_came.at[9])


def gather(train_gate, low_gate, high_gate, train_up, low_up, high_up, norm_train, norm_step):
    rows, width = train_gate.shape
    vmem = pl.BlockSpec(memory_space=pltpu.VMEM)
    smem = pl.BlockSpec(memory_space=pltpu.SMEM)
    dma = pltpu.SemaphoreType.DMA
    return pl.pallas_call(
        gather_kernel,
        name="gather",
        out_shape=(
            pltpu.VMEM((2, CHIPS, rows, width), jnp.bfloat16),
            pltpu.VMEM((2, CHIPS, rows, width), jnp.bfloat16),
            pltpu.VMEM((2, SIDE, SIDE, SIDE, 1, LANES), jnp.float32),
        ),
        in_specs=[vmem] * 6 + [smem] * 2,
        out_specs=(vmem, vmem, vmem),
        scratch_shapes=[dma, dma((20,)), dma, dma] * 2 + [dma((10,)), dma((10,))],
        compiler_params=pltpu.CompilerParams(
            collective_id=0, has_side_effects=True, vmem_limit_bytes=24 * 2**20
        ),
    )(train_gate, low_gate, high_gate, train_up, low_up, high_up, norm_train, norm_step)


STEP = 256
SLOTS = 4


def finish_kernel(gate, up, norm, serve_gate, serve_up, serve_norm, rows, sems):
    serve_norm[...] = jnp.sum(norm[...], axis=(0, 3)).reshape(CHIPS, LANES).astype(jnp.bfloat16)
    steps = gate.shape[-1] // STEP

    def flush(out, i, slot):
        return pltpu.make_async_copy(rows.at[slot], out.at[pl.ds(i * STEP, STEP)], sems.at[slot])

    jobs = [(src, out, i) for src, out in ((gate, serve_gate), (up, serve_up)) for i in range(steps)]
    for n, (src, out, i) in enumerate(jobs):
        slot = n % SLOTS
        if n >= SLOTS:
            flush(*jobs[n - SLOTS][1:], slot).wait()
        for k in range(CHIPS):
            tile = jnp.concatenate(
                [src[0, k, :, pl.ds(i * STEP, STEP)], src[1, k, :, pl.ds(i * STEP, STEP)]], axis=0
            )
            rows[slot, :, pl.ds(k * LANES, LANES)] = tile.T
        flush(out, i, slot).start()
    for n in range(len(jobs) - SLOTS, len(jobs)):
        flush(*jobs[n][1:], n % SLOTS).wait()


def finish(gate, up, norm):
    rows, width = gate.shape[-2:]
    vmem = pl.BlockSpec(memory_space=pltpu.VMEM)
    hbm = pl.BlockSpec(memory_space=pl.ANY)
    wide = 2 * CHIPS * rows
    return pl.pallas_call(
        finish_kernel,
        name="finish",
        out_shape=(
            jax.ShapeDtypeStruct((width, wide), jnp.bfloat16),
            jax.ShapeDtypeStruct((width, wide), jnp.bfloat16),
            jax.ShapeDtypeStruct((CHIPS, LANES), jnp.bfloat16),
        ),
        in_specs=[vmem] * 3,
        out_specs=(hbm, hbm, vmem),
        scratch_shapes=[pltpu.VMEM((SLOTS, STEP, wide), jnp.bfloat16), pltpu.SemaphoreType.DMA((SLOTS,))],
        compiler_params=pltpu.CompilerParams(vmem_limit_bytes=24 * 2**20),
    )(gate, up, norm)


def local(*args):
    serve_gate, serve_up, serve_norm = finish(*gather(*args))
    return serve_gate, serve_up, serve_norm.reshape(-1)


def solution(mesh):
    finer = Mesh(
        mesh.devices.reshape(mesh.shape["trial"], SIDE, SIDE, 2, mesh.shape["cols"]),
        ("trial", "y", "x", "core", "cols"),
    )
    in_specs = (
        P(TRIAL_SHARD, "cols"),
        P(TRIAL_SHARD, None),
        P("trial", "cols"),
        P(TRIAL_SHARD, "cols"),
        P(TRIAL_SHARD, None),
        P("trial", "cols"),
        P(TRIAL_SHARD_COLS),
        P(TRIAL_SHARD_COLS),
    )
    out_specs = (P(("trial", "cols"), None), P(("trial", "cols"), None), P("trial"))
    return jax.shard_map(local, mesh=finer, in_specs=in_specs, out_specs=out_specs, check_vma=False)
```

```python
import functools

import jax
import jax.numpy as jnp
from jax import lax
from jax.experimental import pallas as pl
from jax.experimental.pallas import tpu as pltpu
from jax.sharding import Mesh
from jax.sharding import PartitionSpec as P

TRIAL_SHARD = ("trial", "y", "x", "core")
TRIAL_SHARD_COLS = ("trial", "y", "x", "core", "cols")
MESH_ID = pl.DeviceIdType.MESH
MIX_RATE = 2.0
SIDE = 4
CHIPS = SIDE * SIDE
LANES = 128


def gather_kernel(
    train_gate, low_gate, high_gate, train_up, low_up, high_up, norm_train, norm_step,
    gate, up, norm,
    train, low, high, gain, loaded,
    gate_sent, gate_came, gate_gave, gate_took, up_sent, up_came, up_gave, up_took, norm_sent, norm_came,
):
    y, x, core, col = (lax.axis_index(a) for a in ("y", "x", "core", "cols"))
    sibling = 1 - core

    def wrap(i):
        return lax.rem(i + SIDE, SIDE)

    barrier = pltpu.get_barrier_semaphore()
    partners = [{"cols": wrap(col + k)} for k in (2, 1, 3)]
    partners += [{"x": wrap(x + 1)}, {"x": wrap(x - 1)}, {"y": wrap(y + 1)}, {"y": wrap(y - 1)}, {"core": sibling}]
    for device in partners:
        pl.semaphore_signal(barrier, inc=1, device_id=device, device_id_type=MESH_ID)

    pairs = [
        (train_gate, train.at[0]), (low_gate, low.at[0]), (high_gate, high.at[0]),
        (train_up, train.at[1]), (low_up, low.at[1]), (high_up, high.at[1]),
        (norm_train, gain.at[0]), (norm_step, gain.at[1]),
    ]
    loads = [pltpu.make_async_copy(src, dst, loaded.at[k]) for k, (src, dst) in enumerate(pairs)]
    for load in loads:
        load.start()

    mine = y * SIDE + x
    for k, ref in enumerate((gate, up)):
        for load in loads[3 * k : 3 * k + 3]:
            load.wait()
        product = lax.dot_general(
            low[k], high[k], (((0,), (0,)), ((), ())), preferred_element_type=jnp.float32
        )
        ref[core, mine] = (train[k].astype(jnp.float32) + MIX_RATE * product).astype(jnp.bfloat16)
    for load in loads[6:]:
        load.wait()
    lane = lax.broadcasted_iota(jnp.int32, (1, LANES), 1)
    row = jnp.zeros((1, LANES), jnp.float32)
    first = core * 64 + col * 16
    for i in range(16):
        row = jnp.where(lane == first + i, gain[0, i] + gain[1, i], row)
    norm[core, y, x, col] = row

    pl.semaphore_wait(barrier, len(partners))

    def send(piece, sent, came, device):
        pltpu.make_async_remote_copy(
            src_ref=piece, dst_ref=piece, send_sem=sent, recv_sem=came, device_id=device, device_id_type=MESH_ID
        ).start()

    def arrive(piece, sem):
        pltpu.make_async_copy(piece, piece, sem).wait()

    class Stream:
        def __init__(self, fast_is_x, ref, sent, came, gave, took):
            self.fast_is_x, self.ref = fast_is_x, ref
            self.sent, self.came, self.gave, self.took = sent, came, gave, took

        def block(self, f, s, half=None):
            at_x, at_y = (x + f, y + s) if self.fast_is_x else (x + s, y + f)
            rows = slice(None) if half is None else pl.ds(half * 32, 32)
            return self.ref.at[core, wrap(at_y) * SIDE + wrap(at_x), rows]

        def push(self, along_fast, step, piece, slot):
            axis, at = ("x", x) if along_fast == self.fast_is_x else ("y", y)
            send(piece, self.sent, self.came.at[slot], {axis: wrap(at + step)})

        def share(self, piece):
            send(piece, self.gave, self.took, {"core": sibling})

        def got(self, piece, slot):
            arrive(piece, self.came.at[slot])
            self.share(piece)

        def fast_own(self):
            self.push(True, 1, self.block(0, 0), 0)
            self.push(True, -1, self.block(0, 0), 1)

        def fast_near(self):
            self.got(self.block(-1, 0), 0)
            self.push(True, 1, self.block(-1, 0, 0), 2)
            self.got(self.block(1, 0), 1)
            self.push(True, -1, self.block(1, 0, 1), 3)

        def fast_far(self):
            self.got(self.block(2, 0, 0), 2)
            self.got(self.block(2, 0, 1), 3)

        def slow_own(self, f):
            k = 4 + 4 * (f % SIDE)
            self.push(False, 1, self.block(f, 0), k)
            self.push(False, -1, self.block(f, 0), k + 1)

        def slow_near(self, f):
            k = 4 + 4 * (f % SIDE)
            self.got(self.block(f, -1), k)
            self.got(self.block(f, 1), k + 1)

        def slow_pass(self, f):
            k = 4 + 4 * (f % SIDE)
            self.push(False, 1, self.block(f, -1, 0), k + 2)
            self.push(False, -1, self.block(f, 1, 1), k + 3)

        def slow_far(self, f):
            k = 4 + 4 * (f % SIDE)
            self.got(self.block(f, 2, 0), k + 2)
            self.got(self.block(f, 2, 1), k + 3)

    streams = (
        Stream(True, gate, gate_sent, gate_came, gate_gave, gate_took),
        Stream(False, up, up_sent, up_came, up_gave, up_took),
    )

    def each(method, *args):
        for st in streams:
            getattr(st, method)(*args)

    def norm_send(piece, axis, at, slot):
        for k in (1, 2, 3):
            send(piece, norm_sent.at[slot + k - 1], norm_came.at[slot + k - 1], {axis: wrap(at + k)})

    def norm_arrive(at, piece_at, slot):
        for k in (1, 2, 3):
            arrive(piece_at(wrap(at - k)), norm_came.at[slot + k - 1])

    each("fast_own")
    each("slow_own", 0)
    norm_send(norm.at[core, y, x, col], "cols", col, 0)
    for st in streams:
        st.share(st.block(0, 0))
    each("fast_near")
    norm_arrive(col, lambda i: norm.at[core, y, x, i], 0)
    norm_send(norm.at[core, y, x], "x", x, 3)
    each("slow_own", -1)
    each("slow_own", 1)
    each("slow_near", 0)
    each("fast_far")
    each("slow_own", 2)
    each("slow_pass", 0)
    each("slow_near", -1)
    norm_arrive(x, lambda i: norm.at[core, y, i], 3)
    norm_send(norm.at[core, y], "y", y, 6)
    each("slow_pass", -1)
    each("slow_near", 1)
    each("slow_pass", 1)
    each("slow_near", 2)
    each("slow_pass", 2)
    each("slow_far", 0)
    each("slow_far", -1)
    norm_arrive(y, lambda i: norm.at[core, i], 6)
    send(norm.at[core], norm_sent.at[9], norm_came.at[9], {"core": sibling})
    each("slow_far", 1)
    each("slow_far", 2)

    for st in streams:
        arrive(st.ref.at[core, pl.ds(0, 15)], st.sent)
        arrive(st.ref.at[core], st.gave)
    for piece, slot in ((norm.at[core, y, x, col], 0), (norm.at[core, y, x], 3), (norm.at[core, y], 6)):
        for k in range(3):
            arrive(piece, norm_sent.at[slot + k])
    arrive(norm.at[core], norm_sent.at[9])
    arrive(norm.at[sibling], norm_came.at[9])
    for st in streams:
        arrive(st.ref.at[sibling], st.took)


def gather(train_gate, low_gate, high_gate, train_up, low_up, high_up, norm_train, norm_step):
    rows, width = train_gate.shape
    rank = low_gate.shape[1]
    vmem = pl.BlockSpec(memory_space=pltpu.VMEM)
    hbm = pl.BlockSpec(memory_space=pltpu.HBM)
    dma = pltpu.SemaphoreType.DMA
    return pl.pallas_call(
        gather_kernel,
        name="gather",
        out_shape=(
            pltpu.VMEM((2, CHIPS, rows, width), jnp.bfloat16),
            pltpu.VMEM((2, CHIPS, rows, width), jnp.bfloat16),
            pltpu.VMEM((2, SIDE, SIDE, SIDE, 1, LANES), jnp.float32),
        ),
        in_specs=[hbm] * 8,
        out_specs=(vmem, vmem, vmem),
        scratch_shapes=[
            pltpu.VMEM((2, rows, width), jnp.bfloat16),
            pltpu.VMEM((2, rank, rows), jnp.bfloat16),
            pltpu.VMEM((2, rank, width), jnp.bfloat16),
            pltpu.SMEM((2, 16), jnp.float32),
            dma((8,)),
        ]
        + [dma, dma((20,)), dma, dma] * 2
        + [dma((10,)), dma((10,))],
        compiler_params=pltpu.CompilerParams(
            collective_id=0, has_side_effects=True, vmem_limit_bytes=24 * 2**20
        ),
    )(*(
        pltpu.with_memory_space_constraint(a, pltpu.HBM)
        for a in (train_gate, low_gate.T, high_gate, train_up, low_up.T, high_up, norm_train, norm_step)
    ))


STEP = 256
SLOTS = 4


def finish_kernel(gate, up, norm, serve_gate, serve_up, serve_norm, rows, sems):
    steps = gate.shape[-1] // STEP

    def flush(out, i, slot):
        return pltpu.make_async_copy(rows.at[slot], out.at[pl.ds(i * STEP, STEP)], sems.at[slot])

    jobs = [(src, out, i) for src, out in ((gate, serve_gate), (up, serve_up)) for i in range(steps)]
    for n, (src, out, i) in enumerate(jobs):
        slot = n % SLOTS
        if n >= SLOTS:
            flush(*jobs[n - SLOTS][1:], slot).wait()
        for k in range(CHIPS):
            tile = jnp.concatenate(
                [src[0, k, :, pl.ds(i * STEP, STEP)], src[1, k, :, pl.ds(i * STEP, STEP)]], axis=0
            )
            rows[slot, :, pl.ds(k * LANES, LANES)] = tile.T
        flush(out, i, slot).start()
    serve_norm[...] = jnp.sum(norm[...], axis=(0, 3)).reshape(CHIPS, LANES).astype(jnp.bfloat16)
    for n in range(len(jobs) - SLOTS, len(jobs)):
        flush(*jobs[n][1:], n % SLOTS).wait()


def finish(gate, up, norm):
    rows, width = gate.shape[-2:]
    vmem = pl.BlockSpec(memory_space=pltpu.VMEM)
    hbm = pl.BlockSpec(memory_space=pl.ANY)
    wide = 2 * CHIPS * rows
    return pl.pallas_call(
        finish_kernel,
        name="finish",
        out_shape=(
            jax.ShapeDtypeStruct((width, wide), jnp.bfloat16),
            jax.ShapeDtypeStruct((width, wide), jnp.bfloat16),
            jax.ShapeDtypeStruct((CHIPS, LANES), jnp.bfloat16),
        ),
        in_specs=[vmem] * 3,
        out_specs=(hbm, hbm, vmem),
        scratch_shapes=[pltpu.VMEM((SLOTS, STEP, wide), jnp.bfloat16), pltpu.SemaphoreType.DMA((SLOTS,))],
        compiler_params=pltpu.CompilerParams(vmem_limit_bytes=24 * 2**20),
    )(gate, up, norm)


def local(*args):
    serve_gate, serve_up, serve_norm = finish(*gather(*args))
    return serve_gate, serve_up, serve_norm.reshape(-1)


def solution(mesh):
    finer = Mesh(
        mesh.devices.reshape(mesh.shape["trial"], SIDE, SIDE, 2, mesh.shape["cols"]),
        ("trial", "y", "x", "core", "cols"),
    )
    in_specs = (
        P(TRIAL_SHARD, "cols"),
        P(TRIAL_SHARD, None),
        P("trial", "cols"),
        P(TRIAL_SHARD, "cols"),
        P(TRIAL_SHARD, None),
        P("trial", "cols"),
        P(TRIAL_SHARD_COLS),
        P(TRIAL_SHARD_COLS),
    )
    out_specs = (P(("trial", "cols"), None), P(("trial", "cols"), None), P("trial"))
    return jax.shard_map(local, mesh=finer, in_specs=in_specs, out_specs=out_specs, check_vma=False)
```

```python
import functools

import jax
import jax.numpy as jnp
from jax import lax
from jax.experimental import pallas as pl
from jax.experimental.pallas import tpu as pltpu
from jax.sharding import Mesh
from jax.sharding import PartitionSpec as P

TRIAL_SHARD = ("trial", "y", "x", "core")
TRIAL_SHARD_COLS = ("trial", "y", "x", "core", "cols")
MESH_ID = pl.DeviceIdType.MESH
MIX_RATE = 2.0
SIDE = 4
CHIPS = SIDE * SIDE
LANES = 128


def gather_kernel(
    train_gate, low_gate, high_gate, train_up, low_up, high_up, norm_train, norm_step,
    turned, norm,
    train, low, high, gain, land, loaded, sent, came, gave, took, norm_sent, norm_came,
):
    y, x, core, col = (lax.axis_index(a) for a in ("y", "x", "core", "cols"))
    sibling = 1 - core

    def wrap(i):
        return lax.rem(i + SIDE, SIDE)

    beside, across = col + 1 - 2 * lax.rem(col, 2), wrap(col + 2)
    barrier = pltpu.get_barrier_semaphore()
    partners = [{"cols": across}, {"cols": beside}]
    partners += [{"x": wrap(x + 1)}, {"x": wrap(x - 1)}, {"y": wrap(y + 1)}, {"y": wrap(y - 1)}, {"core": sibling}]
    for device in partners:
        pl.semaphore_signal(barrier, inc=1, device_id=device, device_id_type=MESH_ID)

    pairs = [
        (train_gate, train.at[0]), (low_gate, low.at[0]), (high_gate, high.at[0]),
        (train_up, train.at[1]), (low_up, low.at[1]), (high_up, high.at[1]),
        (norm_train, gain.at[0]), (norm_step, gain.at[1]),
    ]
    loads = [pltpu.make_async_copy(src, dst, loaded.at[k]) for k, (src, dst) in enumerate(pairs)]
    for load in loads:
        load.start()

    mine = y * SIDE + x
    for k in range(2):
        for load in loads[3 * k : 3 * k + 3]:
            load.wait()
        product = lax.dot_general(
            low[k], high[k], (((0,), (0,)), ((), ())), preferred_element_type=jnp.float32
        )
        land[k, core, mine] = (train[k].astype(jnp.float32) + MIX_RATE * product).astype(jnp.bfloat16)
    for load in loads[6:]:
        load.wait()
    lane = lax.broadcasted_iota(jnp.int32, (1, LANES), 1)
    row = jnp.zeros((1, LANES), jnp.float32)
    first = core * 64 + col * 16
    for i in range(16):
        row = jnp.where(lane == first + i, gain[0, i] + gain[1, i], row)
    norm[core, y, x, col] = row

    pl.semaphore_wait(barrier, len(partners))

    def send(piece, sent_sem, came_sem, device):
        pltpu.make_async_remote_copy(
            src_ref=piece, dst_ref=piece, send_sem=sent_sem, recv_sem=came_sem, device_id=device, device_id_type=MESH_ID
        ).start()

    def arrive(piece, sem):
        pltpu.make_async_copy(piece, piece, sem).wait()

    def place(k, f, s):
        at_x, at_y = (x + f, y + s) if k == 0 else (x + s, y + f)
        return wrap(at_y) * SIDE + wrap(at_x)

    def block(k, f, s, at=0, rows=64):
        return land.at[k, core, place(k, f, s), pl.ds(at, rows)]

    def push(k, along_fast, step, piece, slot):
        axis, at = ("x", x) if along_fast == (k == 0) else ("y", y)
        send(piece, sent.at[k], came.at[k, slot], {axis: wrap(at + step)})

    def share(k, piece, group):
        send(piece, gave.at[k], took.at[k, group], {"core": sibling})

    def got(k, piece, slot, group):
        arrive(piece, came.at[k, slot])
        share(k, piece, group)

    def fast_own(k):
        push(k, True, 1, block(k, 0, 0), 0)
        push(k, True, -1, block(k, 0, 0), 1)

    def fast_near(k):
        got(k, block(k, -1, 0), 0, 0)
        push(k, True, 1, block(k, -1, 0, 0, 32), 2)
        got(k, block(k, 1, 0), 1, 0)
        push(k, True, -1, block(k, 1, 0, 32, 32), 3)

    def fast_far(k):
        got(k, block(k, 2, 0, 0, 32), 2, 0)
        got(k, block(k, 2, 0, 32, 32), 3, 0)

    def slow_own(k, f):
        slot = 4 + 4 * (f % SIDE)
        push(k, False, 1, block(k, f, 0), slot)
        push(k, False, -1, block(k, f, 0), slot + 1)

    def slow_near(k, f):
        slot = 4 + 4 * (f % SIDE)
        got(k, block(k, f, -1), slot, 1 + f % SIDE)
        got(k, block(k, f, 1), slot + 1, 1 + f % SIDE)

    def halves(f):
        slot = 4 + 4 * (f % SIDE)
        if f != 2:
            return [(0, 32, slot + 2, 1), (32, 32, slot + 3, -1)]
        return [(0, 16, slot + 2, 1), (32, 16, slot + 3, -1), (16, 16, 20, 1), (48, 16, 21, -1)]

    def slow_pass(k, f):
        for at, rows, slot, step in halves(f):
            push(k, False, step, block(k, f, -step, at, rows), slot)

    def slow_far(k, f):
        for at, rows, slot, _ in halves(f):
            got(k, block(k, f, 2, at, rows), slot, 5 + f % SIDE)

    def each(step, *args):
        for k in range(2):
            step(k, *args)

    def turn(group, chips):
        for k in range(2):
            arrive(land.at[k, sibling, pl.ds(0, len(chips))], took.at[k, group])
            for f, s in chips:
                chip = place(k, f, s)
                lanes = pl.ds(pl.multiple_of(chip * LANES, LANES), LANES)
                tile = jnp.concatenate([land[k, 0, chip], land[k, 1, chip]], axis=0)
                turned[k, :, lanes] = tile.T

    def norm_send(piece, axis, at, slot):
        for k in (1, 2, 3):
            send(piece, norm_sent.at[slot + k - 1], norm_came.at[slot + k - 1], {axis: wrap(at + k)})

    def norm_arrive(at, piece_at, slot):
        for k in (1, 2, 3):
            arrive(piece_at(wrap(at - k)), norm_came.at[slot + k - 1])

    one = norm.at[core, y, x, col]
    pair = norm.at[core, y, x, pl.ds(col - lax.rem(col, 2), 2)]
    other_pair = norm.at[core, y, x, pl.ds(across - lax.rem(across, 2), 2)]
    line, plane = norm.at[core, y, x], norm.at[core, y]

    each(fast_own)
    send(one, norm_sent.at[0], norm_came.at[0], {"cols": beside})
    each(slow_own, 0)
    each(lambda k: share(k, block(k, 0, 0), 0))
    arrive(norm.at[core, y, x, beside], norm_came.at[0])
    send(pair, norm_sent.at[1], norm_came.at[1], {"cols": across})
    each(fast_near)
    arrive(other_pair, norm_came.at[1])
    norm_send(line, "x", x, 2)
    each(slow_own, -1)
    each(slow_own, 1)
    each(slow_near, 0)
    each(fast_far)
    each(slow_own, 2)
    each(slow_pass, 0)
    each(slow_near, -1)
    norm_arrive(x, lambda i: norm.at[core, y, i], 2)
    norm_send(plane, "y", y, 5)
    each(slow_pass, -1)
    turn(0, [(0, 0), (-1, 0), (1, 0), (2, 0)])
    each(slow_near, 1)
    each(slow_pass, 1)
    turn(1, [(0, -1), (0, 1)])
    turn(1 + 3, [(-1, -1), (-1, 1)])
    each(slow_near, 2)
    each(slow_pass, 2)
    turn(1 + 1, [(1, -1), (1, 1)])
    each(slow_far, 0)
    turn(1 + 2, [(2, -1), (2, 1)])
    each(slow_far, -1)
    norm_arrive(y, lambda i: norm.at[core, i], 5)
    send(norm.at[core], norm_sent.at[8], norm_came.at[8], {"core": sibling})
    turn(5, [(0, 2)])
    each(slow_far, 1)
    turn(5 + 3, [(-1, 2)])
    each(slow_far, 2)
    turn(5 + 1, [(1, 2)])

    for k in range(2):
        arrive(land.at[k, core, pl.ds(0, 15)], sent.at[k])
        arrive(land.at[k, core], gave.at[k])
    for piece, slots in ((one, (0,)), (pair, (1,)), (line, (2, 3, 4)), (plane, (5, 6, 7)), (norm.at[core], (8,))):
        for slot in slots:
            arrive(piece, norm_sent.at[slot])
    arrive(norm.at[sibling], norm_came.at[8])
    turn(5 + 2, [(2, 2)])


def gather(train_gate, low_gate, high_gate, train_up, low_up, high_up, norm_train, norm_step):
    rows, width = train_gate.shape
    rank = low_gate.shape[1]
    vmem = pl.BlockSpec(memory_space=pltpu.VMEM)
    hbm = pl.BlockSpec(memory_space=pltpu.HBM)
    dma = pltpu.SemaphoreType.DMA
    return pl.pallas_call(
        gather_kernel,
        name="gather",
        out_shape=(
            pltpu.VMEM((2, width, 2 * CHIPS * rows), jnp.bfloat16),
            pltpu.VMEM((2, SIDE, SIDE, SIDE, 1, LANES), jnp.float32),
        ),
        in_specs=[hbm] * 8,
        out_specs=(vmem, vmem),
        scratch_shapes=[
            pltpu.VMEM((2, rows, width), jnp.bfloat16),
            pltpu.VMEM((2, rank, rows), jnp.bfloat16),
            pltpu.VMEM((2, rank, width), jnp.bfloat16),
            pltpu.SMEM((2, 16), jnp.float32),
            pltpu.VMEM((2, 2, CHIPS, rows, width), jnp.bfloat16),
            dma((8,)),
            dma((2,)), dma((2, 22)), dma((2,)), dma((2, 9)), dma((9,)), dma((9,)),
        ],
        compiler_params=pltpu.CompilerParams(
            collective_id=0, has_side_effects=True, vmem_limit_bytes=28 * 2**20
        ),
    )(*(
        pltpu.with_memory_space_constraint(a, pltpu.HBM)
        for a in (train_gate, low_gate.T, high_gate, train_up, low_up.T, high_up, norm_train, norm_step)
    ))


PIECES = 4


def finish_kernel(turned, norm, serve_gate, serve_up, serve_norm, sems):
    rows = serve_gate.shape[0] // PIECES
    copies = [
        pltpu.make_async_copy(turned.at[k, pl.ds(i * rows, rows)], out.at[pl.ds(i * rows, rows)], sems.at[k, i])
        for k, out in enumerate((serve_gate, serve_up))
        for i in range(PIECES)
    ]
    for copy in copies:
        copy.start()
    serve_norm[...] = jnp.sum(norm[...], axis=(0, 3)).reshape(CHIPS, LANES).astype(jnp.bfloat16)
    for copy in copies:
        copy.wait()


def finish(turned, norm):
    vmem = pl.BlockSpec(memory_space=pltpu.VMEM)
    hbm = pl.BlockSpec(memory_space=pl.ANY)
    return pl.pallas_call(
        finish_kernel,
        name="finish",
        out_shape=(
            jax.ShapeDtypeStruct(turned.shape[1:], jnp.bfloat16),
            jax.ShapeDtypeStruct(turned.shape[1:], jnp.bfloat16),
            jax.ShapeDtypeStruct((CHIPS, LANES), jnp.bfloat16),
        ),
        in_specs=[vmem] * 2,
        out_specs=(hbm, hbm, vmem),
        scratch_shapes=[pltpu.SemaphoreType.DMA((2, PIECES))],
        compiler_params=pltpu.CompilerParams(vmem_limit_bytes=4 * 2**20),
    )(turned, norm)


def local(*args):
    serve_gate, serve_up, serve_norm = finish(*gather(*args))
    return serve_gate, serve_up, serve_norm.reshape(-1)


def solution(mesh):
    finer = Mesh(
        mesh.devices.reshape(mesh.shape["trial"], SIDE, SIDE, 2, mesh.shape["cols"]),
        ("trial", "y", "x", "core", "cols"),
    )
    in_specs = (
        P(TRIAL_SHARD, "cols"),
        P(TRIAL_SHARD, None),
        P("trial", "cols"),
        P(TRIAL_SHARD, "cols"),
        P(TRIAL_SHARD, None),
        P("trial", "cols"),
        P(TRIAL_SHARD_COLS),
        P(TRIAL_SHARD_COLS),
    )
    out_specs = (P(("trial", "cols"), None), P(("trial", "cols"), None), P("trial"))
    return jax.shard_map(local, mesh=finer, in_specs=in_specs, out_specs=out_specs, check_vma=False)
```

```python
import functools

import jax
import jax.numpy as jnp
from jax import lax
from jax.experimental import pallas as pl
from jax.experimental.pallas import tpu as pltpu
from jax.sharding import Mesh
from jax.sharding import PartitionSpec as P

TRIAL_SHARD = ("trial", "y", "x", "core")
TRIAL_SHARD_COLS = ("trial", "y", "x", "core", "cols")
MESH_ID = pl.DeviceIdType.MESH
MIX_RATE = 2.0
SIDE = 4
CHIPS = SIDE * SIDE
LANES = 128


def gather_kernel(
    train_gate, low_gate, high_gate, train_up, low_up, high_up, norm_train, norm_step,
    turned, whole_gain,
    train, low, high, gain, norm, land, loaded, sent, came, gave, took, norm_sent, norm_came,
):
    y, x, core, col = (lax.axis_index(a) for a in ("y", "x", "core", "cols"))
    sibling = 1 - core

    def wrap(i):
        return lax.rem(i + SIDE, SIDE)

    width = train.shape[2]
    half = width // 2
    beside, across = col + 1 - 2 * lax.rem(col, 2), wrap(col + 2)
    barrier = pltpu.get_barrier_semaphore()
    partners = [{"cols": across}, {"cols": beside}]
    partners += [{"x": wrap(x + 1)}, {"x": wrap(x - 1)}, {"y": wrap(y + 1)}, {"y": wrap(y - 1)}, {"core": sibling}]
    for device in partners:
        pl.semaphore_signal(barrier, inc=1, device_id=device, device_id_type=MESH_ID)

    pairs = [
        (train_gate, train.at[0]), (low_gate, low.at[0]), (high_gate, high.at[0]),
        (train_up, train.at[1]), (low_up, low.at[1]), (high_up, high.at[1]),
        (norm_train, gain.at[0]), (norm_step, gain.at[1]),
    ]
    loads = [pltpu.make_async_copy(src, dst, loaded.at[k]) for k, (src, dst) in enumerate(pairs)]
    for load in loads:
        load.start()

    def merge(k):
        for load in loads[3 * k : 3 * k + 3]:
            load.wait()
        product = lax.dot_general(
            low[k], high[k], (((0,), (0,)), ((), ())), preferred_element_type=jnp.float32
        )
        merged = train[k].astype(jnp.float32) + MIX_RATE * product
        land[k, core, y * SIDE + x] = merged.astype(jnp.bfloat16)

    merge(0)
    for load in loads[6:]:
        load.wait()
    lane = lax.broadcasted_iota(jnp.int32, (1, LANES), 1)
    row = jnp.zeros((1, LANES), jnp.float32)
    first = core * 64 + col * 16
    for i in range(16):
        row = jnp.where(lane == first + i, gain[0, i] + gain[1, i], row)
    norm[core, y, x, col] = row
    pl.semaphore_wait(barrier, len(partners))

    def send(piece, sent_sem, came_sem, device):
        pltpu.make_async_remote_copy(
            src_ref=piece, dst_ref=piece, send_sem=sent_sem, recv_sem=came_sem, device_id=device, device_id_type=MESH_ID
        ).start()

    def arrive(piece, sem):
        pltpu.make_async_copy(piece, piece, sem).wait()

    def place(k, f, s):
        at_x, at_y = (x + f, y + s) if k == 0 else (x + s, y + f)
        return wrap(at_y) * SIDE + wrap(at_x)

    def block(k, f, s, at=0, width=width):
        return land.at[k, core, place(k, f, s), :, pl.ds(at, width)]

    def push(k, along_fast, step, piece, slot):
        axis, at = ("x", x) if along_fast == (k == 0) else ("y", y)
        send(piece, sent, came.at[k, slot], {axis: wrap(at + step)})

    def share(piece, group):
        send(piece, gave, took.at[group], {"core": sibling})

    def fast_own(k):
        for step in (1, -1):
            push(k, True, step, block(k, 0, 0), 0)

    def fast_near(k):
        arrive(land.at[k, core, pl.ds(0, 2)], came.at[k, 0])
        push(k, True, 1, block(k, -1, 0, 0, half), 1)
        push(k, True, -1, block(k, 1, 0, half, half), 1)
        for f in (-1, 1):
            share(block(k, f, 0), 0)

    def fast_far(k):
        arrive(land.at[k, core, 0], came.at[k, 1])
        share(block(k, 2, 0), 0)

    def slow_own(k, f):
        for step in (1, -1):
            push(k, False, step, block(k, f, 0), 2 + f % SIDE)

    def slow_near(k, f):
        arrive(land.at[k, core, pl.ds(0, 2)], came.at[k, 2 + f % SIDE])
        for s in (-1, 1):
            share(block(k, f, s), 1 + f % SIDE)

    def slow_pass(k, f, at=0, size=half, slot=None):
        for step, start in ((1, at), (-1, half + at)):
            push(k, False, step, block(k, f, -step, start, size), slot or 6 + f % SIDE)

    def slow_far(k, f):
        arrive(land.at[k, core, 0], came.at[k, 6 + f % SIDE])
        share(block(k, f, 2), 5 + f % SIDE)

    def last_far(k, at, slot, group):
        arrive(land.at[k, core, 0, :, pl.ds(0, half)], came.at[k, slot])
        for start in (at, half + at):
            share(block(k, 2, 2, start, half // 2), group)

    def each(step, *args):
        for k in range(2):
            step(k, *args)

    def turn(group, chips, ranges=None, amount=width):
        arrive(land.at[:, sibling, pl.ds(0, len(chips)), :, pl.ds(0, amount)], took.at[group])
        for k in range(2):
            for f, s in chips:
                chip = place(k, f, s)
                lanes = pl.ds(pl.multiple_of(chip * LANES, LANES), LANES)
                for at, size in ranges or [(0, width)]:
                    tile = [land[k, c, chip, :, pl.ds(at, size)] for c in range(2)]
                    turned[k, pl.ds(at, size), lanes] = jnp.concatenate(tile, axis=0).T

    def norm_send(piece, axis, at, slot):
        for k in (1, 2, 3):
            send(piece, norm_sent.at[slot], norm_came.at[slot], {axis: wrap(at + k)})

    one = norm.at[core, y, x, col]
    pair = norm.at[core, y, x, pl.ds(col - lax.rem(col, 2), 2)]
    other_pair = norm.at[core, y, x, pl.ds(across - lax.rem(across, 2), 2)]
    three_lines, three_planes = norm.at[core, y, pl.ds(0, 3)], norm.at[core, pl.ds(0, 3)]

    fast_own(0)
    slow_own(0, 0)
    send(one, norm_sent.at[0], norm_came.at[0], {"cols": beside})
    merge(1)
    share(block(0, 0, 0), 0)
    arrive(norm.at[core, y, x, beside], norm_came.at[0])
    fast_own(1)
    slow_own(1, 0)
    send(pair, norm_sent.at[1], norm_came.at[1], {"cols": across})
    share(block(1, 0, 0), 0)
    fast_near(0)
    arrive(other_pair, norm_came.at[1])
    norm_send(norm.at[core, y, x], "x", x, 2)
    slow_own(0, -1)
    slow_near(0, 0)
    fast_near(1)
    slow_near(1, 0)
    slow_own(0, 1)
    slow_pass(1, 0)
    slow_own(1, -1)
    slow_own(1, 1)
    fast_far(0)
    slow_own(0, 2)
    slow_pass(0, 0)
    slow_near(0, -1)
    fast_far(1)
    slow_own(1, 2)
    slow_near(1, -1)
    arrive(three_lines, norm_came.at[2])
    norm_send(norm.at[core, y], "y", y, 3)
    each(slow_pass, -1)
    each(slow_near, 1)
    each(slow_pass, 1)
    turn(0, [(0, 0), (-1, 0), (1, 0), (2, 0)])
    each(slow_near, 2)
    each(slow_pass, 2, 0, half // 2)
    each(slow_pass, 2, half // 2, half // 2, 10)
    turn(1, [(0, -1), (0, 1)])
    turn(1 + 3, [(-1, -1), (-1, 1)])
    each(slow_far, 0)
    turn(1 + 1, [(1, -1), (1, 1)])
    each(slow_far, -1)
    turn(1 + 2, [(2, -1), (2, 1)])
    arrive(three_planes, norm_came.at[3])
    send(norm.at[core], norm_sent.at[4], norm_came.at[4], {"core": sibling})
    turn(5, [(0, 2)])
    each(slow_far, 1)
    turn(5 + 3, [(-1, 2)])
    arrive(norm.at[sibling], norm_came.at[4])
    whole_gain[...] = jnp.sum(norm[...], axis=(0, 3)).reshape(CHIPS, LANES).astype(jnp.bfloat16)
    each(last_far, 0, 6 + 2, 5 + 2)
    each(last_far, half // 2, 10, 9)
    turn(5 + 1, [(1, 2)])
    turn(5 + 2, [(2, 2)], [(0, half // 2), (half, half // 2)], half)
    turn(9, [(2, 2)], [(half // 2, half // 2), (3 * half // 2, half // 2)], half)

    arrive(land.at[:, core, pl.ds(0, 15)], sent)
    arrive(land.at[:, core], gave)
    for slot, piece in enumerate((one, pair, three_lines, three_planes, norm.at[core])):
        arrive(piece, norm_sent.at[slot])


def gather(train_gate, low_gate, high_gate, train_up, low_up, high_up, norm_train, norm_step):
    rows, width = train_gate.shape
    rank = low_gate.shape[1]
    vmem = pl.BlockSpec(memory_space=pltpu.VMEM)
    hbm = pl.BlockSpec(memory_space=pltpu.HBM)
    dma = pltpu.SemaphoreType.DMA
    return pl.pallas_call(
        gather_kernel,
        name="gather",
        out_shape=(
            pltpu.VMEM((2, width, 2 * CHIPS * rows), jnp.bfloat16),
            pltpu.VMEM((CHIPS, LANES), jnp.bfloat16),
        ),
        in_specs=[hbm] * 8,
        out_specs=(vmem, vmem),
        scratch_shapes=[
            pltpu.VMEM((2, rows, width), jnp.bfloat16),
            pltpu.VMEM((2, rank, rows), jnp.bfloat16),
            pltpu.VMEM((2, rank, width), jnp.bfloat16),
            pltpu.SMEM((2, 16), jnp.float32),
            pltpu.VMEM((2, SIDE, SIDE, SIDE, 1, LANES), jnp.float32),
            pltpu.VMEM((2, 2, CHIPS, rows, width), jnp.bfloat16),
            dma((8,)), dma, dma((2, 11)), dma, dma((10,)), dma((5,)), dma((5,)),
        ],
        compiler_params=pltpu.CompilerParams(
            collective_id=0, has_side_effects=True, vmem_limit_bytes=28 * 2**20
        ),
    )(*(
        pltpu.with_memory_space_constraint(a, pltpu.HBM)
        for a in (train_gate, low_gate.T, high_gate, train_up, low_up.T, high_up, norm_train, norm_step)
    ))


def finish_kernel(turned, gain, serve_gate, serve_up, serve_norm, sems):
    rows = serve_gate.shape[0] // 2
    halves = [pl.ds(i * rows, rows) for i in range(2)]
    pairs = [(turned.at[k, h], out.at[h]) for k, out in enumerate((serve_gate, serve_up)) for h in halves]
    pairs.append((gain, serve_norm))
    copies = [pltpu.make_async_copy(src, dst, sems.at[k]) for k, (src, dst) in enumerate(pairs)]
    for copy in copies:
        copy.start()
    for copy in copies:
        copy.wait()


def finish(turned, gain):
    vmem = pl.BlockSpec(memory_space=pltpu.VMEM)
    hbm = pl.BlockSpec(memory_space=pl.ANY)
    return pl.pallas_call(
        finish_kernel,
        name="finish",
        out_shape=(
            jax.ShapeDtypeStruct(turned.shape[1:], jnp.bfloat16),
            jax.ShapeDtypeStruct(turned.shape[1:], jnp.bfloat16),
            jax.ShapeDtypeStruct(gain.shape, jnp.bfloat16),
        ),
        in_specs=[vmem] * 2,
        out_specs=(hbm, hbm, hbm),
        scratch_shapes=[pltpu.SemaphoreType.DMA((5,))],
        compiler_params=pltpu.CompilerParams(vmem_limit_bytes=4 * 2**20),
    )(turned, gain)


def local(*args):
    serve_gate, serve_up, serve_norm = finish(*gather(*args))
    return serve_gate, serve_up, serve_norm.reshape(-1)


def solution(mesh):
    finer = Mesh(
        mesh.devices.reshape(mesh.shape["trial"], SIDE, SIDE, 2, mesh.shape["cols"]),
        ("trial", "y", "x", "core", "cols"),
    )
    in_specs = (
        P(TRIAL_SHARD, "cols"),
        P(TRIAL_SHARD, None),
        P("trial", "cols"),
        P(TRIAL_SHARD, "cols"),
        P(TRIAL_SHARD, None),
        P("trial", "cols"),
        P(TRIAL_SHARD_COLS),
        P(TRIAL_SHARD_COLS),
    )
    out_specs = (P(("trial", "cols"), None), P(("trial", "cols"), None), P("trial"))
    return jax.shard_map(local, mesh=finer, in_specs=in_specs, out_specs=out_specs, check_vma=False)
```

```python
import functools

import jax
import jax.numpy as jnp
from jax import lax
from jax.experimental import pallas as pl
from jax.experimental.pallas import tpu as pltpu
from jax.sharding import Mesh
from jax.sharding import PartitionSpec as P

TRIAL_SHARD = ("trial", "y", "x", "core")
TRIAL_SHARD_COLS = ("trial", "y", "x", "core", "cols")
MESH_ID = pl.DeviceIdType.MESH
MIX_RATE = 2.0
SIDE = 4
CHIPS = SIDE * SIDE
LANES = 128


def gather_kernel(
    train_gate, low_gate, high_gate, train_up, low_up, high_up, norm_train, norm_step,
    turned, whole_gain,
    train, low, high, gain, norm, land, loaded, sent, came, gave, took, norm_came,
):
    y, x, core, col = (lax.axis_index(a) for a in ("y", "x", "core", "cols"))
    sibling = 1 - core
    width = train.shape[2]
    half, quarter, tail = width // 2, width // 4, width // 8

    def wrap(i):
        return lax.rem(i + SIDE, SIDE)

    pairs = [
        (train_gate, train.at[0]), (high_gate, high.at[0]), (low_gate, low.at[0]),
        (train_up, train.at[1]), (high_up, high.at[1]), (low_up, low.at[1]),
        (norm_train, gain.at[0]), (norm_step, gain.at[1]),
    ]
    loads = [pltpu.make_async_copy(src, dst, loaded.at[k]) for k, (src, dst) in enumerate(pairs)]
    for load in loads[:3]:
        load.start()

    beside, across = col + 1 - 2 * lax.rem(col, 2), wrap(col + 2)
    barrier = pltpu.get_barrier_semaphore()
    partners = [{"cols": across}, {"x": wrap(x + 1)}, {"x": wrap(x - 1)}, {"y": wrap(y + 1)}, {"y": wrap(y - 1)}]
    partners += [{"cols": beside}, {"core": sibling}]
    for device in partners:
        pl.semaphore_signal(barrier, inc=1, device_id=device, device_id_type=MESH_ID)
    for load in loads[3:]:
        load.start()

    def send(piece, sent_sem, came_sem, device):
        pltpu.make_async_remote_copy(
            src_ref=piece, dst_ref=piece, send_sem=sent_sem, recv_sem=came_sem, device_id=device, device_id_type=MESH_ID
        ).start()

    def arrive(piece, sem):
        pltpu.make_async_copy(piece, piece, sem).wait()

    def merge(k, at, size):
        product = lax.dot_general(
            low[k], high[k, :, pl.ds(at, size)], (((0,), (0,)), ((), ())), preferred_element_type=jnp.float32
        )
        merged = train[k, :, pl.ds(at, size)].astype(jnp.float32) + MIX_RATE * product
        land[k, core, y * SIDE + x, :, pl.ds(at, size)] = merged.astype(jnp.bfloat16)

    def place(k, f, s):
        at_x, at_y = (x + f, y + s) if k == 0 else (x + s, y + f)
        return wrap(at_y) * SIDE + wrap(at_x)

    def block(k, f, s, at=0, size=width, side=core):
        return land.at[k, side, place(k, f, s), :, pl.ds(at, size)]

    def push(k, along_fast, step, piece, slot, kind=0):
        axis, at = ("x", x) if along_fast == (k == 0) else ("y", y)
        send(piece, sent.at[kind], came.at[slot], {axis: wrap(at + step)})

    def share(piece, group, kind=0):
        send(piece, gave.at[kind], took.at[group], {"core": sibling})

    def own(k, at=0, size=width):
        for along_fast, slot in ((True, 6 * k), (False, 6 * k + 2)):
            for step in (1, -1):
                push(k, along_fast, step, block(k, 0, 0, at, size), slot)

    def fast_near(k):
        arrive(land.at[k, core, pl.ds(0, 2)], came.at[6 * k])
        push(k, True, 1, block(k, -1, 0, 0, half), 6 * k + 1)
        push(k, True, -1, block(k, 1, 0, half, half), 6 * k + 1)
        for f in (-1, 1):
            share(block(k, f, 0), 0)

    def fast_far(k):
        arrive(land.at[k, core, 0], came.at[6 * k + 1])
        share(block(k, 2, 0), 0)

    def slow_own(k, f):
        for step in (1, -1):
            push(k, False, step, block(k, f, 0), 6 * k + 2 + f % SIDE)

    def slow_near(k, f):
        arrive(land.at[k, core, pl.ds(0, 2)], came.at[6 * k + 2 + f % SIDE])
        for s in (-1, 1):
            share(block(k, f, s), {0: 0, -1: 0, 1: 1, 2: 2}[f])

    def slow_pass(k, f, slot, at=0, size=half, side=core):
        for step, start in ((1, at), (-1, half + at)):
            push(k, False, step, block(k, f, -step, start, size, side), slot, int(f == 0))

    def slow_far(slot, count, size, pieces, group, kind=0):
        arrive(land.at[:, core, pl.ds(0, count), :, pl.ds(0, size)], came.at[slot])
        for k in range(2):
            for f, starts, length, side in pieces:
                for start in starts:
                    share(block(k, f, 2, start, length, side), group, int(f == 0))

    def theirs(group, blocks, size=width):
        arrive(land.at[:, sibling, pl.ds(0, blocks), :, pl.ds(0, size)], took.at[group])

    def turn(chips, ranges=((0, width),)):
        for k in range(2):
            for f, s in chips:
                chip = place(k, f, s)
                lanes = pl.ds(pl.multiple_of(chip * LANES, LANES), LANES)
                for at, size in ranges:
                    tile = [land[k, c, chip, :, pl.ds(at, size)] for c in range(2)]
                    turned[k, pl.ds(at, size), lanes] = jnp.concatenate(tile, axis=0).T

    def norm_send(pieces, slot):
        for piece, device in pieces:
            send(piece, loaded.at[slot], norm_came.at[slot], device)

    one = norm.at[core, y, x, col]
    pair = norm.at[core, y, x, pl.ds(col - lax.rem(col, 2), 2)]
    other_pair = norm.at[core, y, x, pl.ds(across - lax.rem(across, 2), 2)]
    three_lines, three_planes = norm.at[core, y, pl.ds(0, 3)], norm.at[core, pl.ds(0, 3)]

    for load in loads[:3]:
        load.wait()
    merge(0, 0, half)
    pl.semaphore_wait(barrier, len(partners))
    own(0, 0, half)
    merge(0, half, half)
    own(0, half, half)

    for load in loads[3:]:
        load.wait()
    lane = lax.broadcasted_iota(jnp.int32, (1, LANES), 1)
    row = jnp.zeros((1, LANES), jnp.float32)
    first = core * 64 + col * 16
    for i in range(16):
        row = jnp.where(lane == first + i, gain[0, i] + gain[1, i], row)
    norm[core, y, x, col] = row
    merge(1, 0, width)
    norm_send([(one, {"cols": beside})], 0)
    own(1)
    for k in range(2):
        share(block(k, 0, 0), 0)
    arrive(norm.at[core, y, x, beside], norm_came.at[0])
    norm_send([(pair, {"cols": across})], 1)

    firsts, seconds = (0, half), (quarter, half + quarter)
    first_ranges, second_ranges = [[(at, quarter) for at in starts] for starts in (firsts, seconds)]
    last = (half - tail, width - tail)

    fast_near(0)
    arrive(other_pair, norm_came.at[1])
    norm_send([(norm.at[core, y, x], {"x": wrap(x + i)}) for i in (1, 2, 3)], 2)
    slow_own(0, -1)
    slow_near(0, 0)
    fast_near(1)
    slow_near(1, 0)
    slow_own(0, 1)
    slow_pass(1, 0, 12, 0, quarter)
    slow_own(1, -1)
    slow_own(1, 1)
    fast_far(0)
    slow_own(0, 2)
    slow_pass(0, 0, 12, 0, quarter)
    slow_near(0, -1)
    fast_far(1)
    slow_own(1, 2)
    slow_near(1, -1)
    arrive(three_lines, norm_came.at[2])
    norm_send([(norm.at[core, y], {"y": wrap(y + i)}) for i in (1, 2, 3)], 3)
    for k in range(2):
        slow_pass(k, -1, 12)
    for k in range(2):
        slow_near(k, 1)
        slow_pass(k, 1, 14)
    theirs(0, 8)

    @pl.when(core == 1)
    def _():
        for k in range(2):
            slow_pass(k, 0, 13, quarter, quarter)
            slow_pass(k, 0, 13, quarter, quarter, sibling)

    turn([(0, 0), (-1, 0), (1, 0), (2, 0)])
    slow_near(0, 2)
    slow_pass(0, 2, 15, 0, half - tail)
    slow_pass(0, 2, 16, half - tail, tail)
    turn([(0, -1), (0, 1)])
    slow_near(1, 2)
    slow_pass(1, 2, 15, 0, half - tail)
    slow_pass(1, 2, 16, half - tail, tail)
    turn([(-1, -1), (-1, 1)])
    theirs(1, 2)
    slow_far(12, 3, half, [(-1, (0,), width, core), (0, firsts, quarter, core)], 3)
    turn([(1, -1), (1, 1)])
    arrive(three_planes, norm_came.at[3])
    norm_send([(norm.at[core], {"core": sibling})], 4)

    theirs(2, 2)
    turn([(2, -1), (2, 1)])
    slow_far(14, 1, width, [(1, (0,), width, core)], 4)

    @pl.when(core == 1)
    def _():
        slow_far(13, 1, width, [(0, seconds, quarter, core), (0, seconds, quarter, sibling)], 6)

    slow_far(15, 1, width - 2 * tail, [(2, firsts, half - tail, core)], 5)
    theirs(3, 3, half)
    turn([(-1, 2)])
    turn([(0, 2)], first_ranges)
    slow_far(16, 1, 2 * tail, [(2, last, tail, core)], 7)
    arrive(norm.at[sibling], norm_came.at[4])
    whole_gain[...] = jnp.sum(norm[...], axis=(0, 3)).reshape(CHIPS, LANES).astype(jnp.bfloat16)

    @pl.when(core == 1)
    def _():
        arrive(land.at[:, core, pl.ds(0, 3), :, pl.ds(0, half)], sent.at[1])
        arrive(land.at[:, core, pl.ds(0, 3), :, pl.ds(0, half)], gave.at[1])

    @pl.when(core == 0)
    def _():
        arrive(land.at[:, core, pl.ds(0, 1), :, pl.ds(0, half)], sent.at[1])
        arrive(land.at[:, core, pl.ds(0, 1), :, pl.ds(0, half)], gave.at[1])
        theirs(6, 1)

    turn([(0, 2)], second_ranges)
    theirs(4, 1)
    turn([(1, 2)])
    theirs(5, 1, width - 2 * tail)
    turn([(2, 2)], [(at, half - tail) for at in firsts])
    theirs(7, 1, 2 * tail)
    turn([(2, 2)], [(at, tail) for at in last])
    arrive(land.at[:, core, pl.ds(0, 14)], sent.at[0])
    arrive(land.at[:, core, pl.ds(0, 15)], gave.at[0])
    for slot, piece in enumerate((one, pair, three_lines, three_planes, norm.at[core])):
        arrive(piece, loaded.at[slot])


def gather(train_gate, low_gate, high_gate, train_up, low_up, high_up, norm_train, norm_step):
    rows, width = train_gate.shape
    rank = low_gate.shape[1]
    vmem = pl.BlockSpec(memory_space=pltpu.VMEM)
    hbm = pl.BlockSpec(memory_space=pltpu.HBM)
    dma = pltpu.SemaphoreType.DMA
    return pl.pallas_call(
        gather_kernel,
        name="gather",
        out_shape=(
            pltpu.VMEM((2, width, 2 * CHIPS * rows), jnp.bfloat16),
            pltpu.VMEM((CHIPS, LANES), jnp.bfloat16),
        ),
        in_specs=[hbm] * 8,
        out_specs=(vmem, vmem),
        scratch_shapes=[
            pltpu.VMEM((2, rows, width), jnp.bfloat16),
            pltpu.VMEM((2, rank, rows), jnp.bfloat16),
            pltpu.VMEM((2, rank, width), jnp.bfloat16),
            pltpu.SMEM((2, 16), jnp.float32),
            pltpu.VMEM((2, SIDE, SIDE, SIDE, 1, LANES), jnp.float32),
            pltpu.VMEM((2, 2, CHIPS, rows, width), jnp.bfloat16),
            dma((8,)), dma((2,)), dma((17,)), dma((2,)), dma((8,)), dma((5,)),
        ],
        compiler_params=pltpu.CompilerParams(
            collective_id=0, has_side_effects=True, vmem_limit_bytes=28 * 2**20
        ),
    )(*(
        pltpu.with_memory_space_constraint(a, pltpu.HBM)
        for a in (train_gate, low_gate.T, high_gate, train_up, low_up.T, high_up, norm_train, norm_step)
    ))


def finish_kernel(turned, gain, serve_gate, serve_up, serve_norm, sems):
    rows = serve_gate.shape[0] // 2
    halves = [pl.ds(i * rows, rows) for i in range(2)]
    pairs = [(turned.at[k, h], out.at[h]) for k, out in enumerate((serve_gate, serve_up)) for h in halves]
    pairs.append((gain, serve_norm))
    copies = [pltpu.make_async_copy(src, dst, sems.at[k]) for k, (src, dst) in enumerate(pairs)]
    for copy in copies:
        copy.start()
    for copy in copies:
        copy.wait()


def finish(turned, gain):
    vmem = pl.BlockSpec(memory_space=pltpu.VMEM)
    hbm = pl.BlockSpec(memory_space=pl.ANY)
    return pl.pallas_call(
        finish_kernel,
        name="finish",
        out_shape=(
            jax.ShapeDtypeStruct(turned.shape[1:], jnp.bfloat16),
            jax.ShapeDtypeStruct(turned.shape[1:], jnp.bfloat16),
            jax.ShapeDtypeStruct(gain.shape, jnp.bfloat16),
        ),
        in_specs=[vmem] * 2,
        out_specs=(hbm, hbm, hbm),
        scratch_shapes=[pltpu.SemaphoreType.DMA((5,))],
        compiler_params=pltpu.CompilerParams(vmem_limit_bytes=4 * 2**20),
    )(turned, gain)


def local(*args):
    serve_gate, serve_up, serve_norm = finish(*gather(*args))
    return serve_gate, serve_up, serve_norm.reshape(-1)


def solution(mesh):
    finer = Mesh(
        mesh.devices.reshape(mesh.shape["trial"], SIDE, SIDE, 2, mesh.shape["cols"]),
        ("trial", "y", "x", "core", "cols"),
    )
    in_specs = (
        P(TRIAL_SHARD, "cols"),
        P(TRIAL_SHARD, None),
        P("trial", "cols"),
        P(TRIAL_SHARD, "cols"),
        P(TRIAL_SHARD, None),
        P("trial", "cols"),
        P(TRIAL_SHARD_COLS),
        P(TRIAL_SHARD_COLS),
    )
    out_specs = (P(("trial", "cols"), None), P(("trial", "cols"), None), P("trial"))
    return jax.shard_map(local, mesh=finer, in_specs=in_specs, out_specs=out_specs, check_vma=False)
```

```python
import functools

import jax
import jax.numpy as jnp
from jax import lax
from jax.experimental import pallas as pl
from jax.experimental.pallas import tpu as pltpu
from jax.sharding import Mesh
from jax.sharding import PartitionSpec as P

TRIAL_SHARD = ("trial", "y", "x", "core")
TRIAL_SHARD_COLS = ("trial", "y", "x", "core", "cols")
MESH_ID = pl.DeviceIdType.MESH
MIX_RATE = 2.0
SIDE = 4
CHIPS = SIDE * SIDE
LANES = 128


def gather_kernel(
    train_gate, low_gate, high_gate, train_up, low_up, high_up, norm_train, norm_step,
    turned, whole_gain,
    train, low, high, gain, norm, land, loaded, sent, came, gave, took, norm_came,
):
    y, x, core, col = (lax.axis_index(a) for a in ("y", "x", "core", "cols"))
    sibling = 1 - core
    width = train.shape[2]
    half, quarter, tail = width // 2, width // 4, width // 8

    def wrap(i):
        return lax.rem(i + SIDE, SIDE)

    pairs = [
        (train_gate, train.at[0]), (high_gate, high.at[0]), (low_gate, low.at[0]),
        (train_up, train.at[1]), (high_up, high.at[1]), (low_up, low.at[1]),
        (norm_train, gain.at[0]), (norm_step, gain.at[1]),
    ]
    loads = [pltpu.make_async_copy(src, dst, loaded.at[k]) for k, (src, dst) in enumerate(pairs)]
    for load in loads[:3]:
        load.start()

    beside, across = col + 1 - 2 * lax.rem(col, 2), wrap(col + 2)
    barrier = pltpu.get_barrier_semaphore()
    partners = [{"cols": across}, {"x": wrap(x + 1)}, {"x": wrap(x - 1)}, {"y": wrap(y + 1)}, {"y": wrap(y - 1)}]
    partners += [{"cols": beside}, {"core": sibling}]
    for device in partners:
        pl.semaphore_signal(barrier, inc=1, device_id=device, device_id_type=MESH_ID)
    for load in loads[3:]:
        load.start()

    def send(piece, sent_sem, came_sem, device):
        pltpu.make_async_remote_copy(
            src_ref=piece, dst_ref=piece, send_sem=sent_sem, recv_sem=came_sem, device_id=device, device_id_type=MESH_ID
        ).start()

    def arrive(piece, sem):
        pltpu.make_async_copy(piece, piece, sem).wait()

    def merge(k, at, size):
        product = lax.dot_general(
            low[k], high[k, :, pl.ds(at, size)], (((0,), (0,)), ((), ())), preferred_element_type=jnp.float32
        )
        merged = train[k, :, pl.ds(at, size)].astype(jnp.float32) + MIX_RATE * product
        land[k, core, y * SIDE + x, :, pl.ds(at, size)] = merged.astype(jnp.bfloat16)

    def place(k, f, s):
        at_x, at_y = (x + f, y + s) if k == 0 else (x + s, y + f)
        return wrap(at_y) * SIDE + wrap(at_x)

    def block(k, f, s, at=0, size=width, side=core):
        return land.at[k, side, place(k, f, s), :, pl.ds(at, size)]

    def push(k, along_fast, step, piece, slot, kind=0):
        axis, at = ("x", x) if along_fast == (k == 0) else ("y", y)
        send(piece, sent.at[kind], came.at[slot], {axis: wrap(at + step)})

    def share(piece, group, kind=0):
        send(piece, gave.at[kind], took.at[group], {"core": sibling})

    def own(k, at=0, size=width):
        for along_fast, slot in ((True, 6 * k), (False, 6 * k + 2)):
            for step in (1, -1):
                push(k, along_fast, step, block(k, 0, 0, at, size), slot)

    def fast_near(k):
        arrive(land.at[k, core, pl.ds(0, 2)], came.at[6 * k])
        push(k, True, 1, block(k, -1, 0, 0, half), 6 * k + 1)
        push(k, True, -1, block(k, 1, 0, half, half), 6 * k + 1)
        for f in (-1, 1):
            share(block(k, f, 0), 0)

    def fast_far(k):
        arrive(land.at[k, core, 0], came.at[6 * k + 1])
        share(block(k, 2, 0), 0)

    def slow_own(k, f):
        for step in (1, -1):
            push(k, False, step, block(k, f, 0), 6 * k + 2 + f % SIDE)

    def slow_near(k, f):
        arrive(land.at[k, core, pl.ds(0, 2)], came.at[6 * k + 2 + f % SIDE])
        for s in (-1, 1):
            share(block(k, f, s), {0: 0, -1: 0, 1: 1, 2: 2}[f])

    def slow_pass(k, f, slot, at=0, size=half, side=core):
        for step, start in ((1, at), (-1, half + at)):
            push(k, False, step, block(k, f, -step, start, size, side), slot, int(f == 0))

    def slow_far(slot, count, size, pieces, group, kind=0):
        arrive(land.at[:, core, pl.ds(0, count), :, pl.ds(0, size)], came.at[slot])
        for k in range(2):
            for f, starts, length, side in pieces:
                for start in starts:
                    share(block(k, f, 2, start, length, side), group, int(f == 0))

    def last_far(k, slot, starts, size, group):
        arrive(land.at[k, core, 0, :, pl.ds(0, 2 * size)], came.at[slot + k])
        for start in starts:
            share(block(k, 2, 2, start, size), group)

    def theirs(group, blocks, size=width):
        arrive(land.at[:, sibling, pl.ds(0, blocks), :, pl.ds(0, size)], took.at[group])

    def turn(chips, ranges=((0, width),)):
        for k in range(2):
            for f, s in chips:
                chip = place(k, f, s)
                lanes = pl.ds(pl.multiple_of(chip * LANES, LANES), LANES)
                for at, size in ranges:
                    tile = [land[k, c, chip, :, pl.ds(at, size)] for c in range(2)]
                    turned[k, pl.ds(at, size), lanes] = jnp.concatenate(tile, axis=0).T

    def norm_send(pieces, slot):
        for piece, device in pieces:
            send(piece, loaded.at[slot], norm_came.at[slot], device)

    one = norm.at[core, y, x, col]
    pair = norm.at[core, y, x, pl.ds(col - lax.rem(col, 2), 2)]
    other_pair = norm.at[core, y, x, pl.ds(across - lax.rem(across, 2), 2)]
    three_lines, three_planes = norm.at[core, y, pl.ds(0, 3)], norm.at[core, pl.ds(0, 3)]

    for load in loads[:3]:
        load.wait()
    merge(0, 0, half)
    pl.semaphore_wait(barrier, len(partners))
    own(0, 0, half)
    merge(0, half, half)
    own(0, half, half)

    for load in loads[3:]:
        load.wait()
    lane = lax.broadcasted_iota(jnp.int32, (1, LANES), 1)
    row = jnp.zeros((1, LANES), jnp.float32)
    first = core * 64 + col * 16
    for i in range(16):
        row = jnp.where(lane == first + i, gain[0, i] + gain[1, i], row)
    norm[core, y, x, col] = row
    merge(1, 0, width)
    norm_send([(one, {"cols": beside})], 0)
    own(1)
    for k in range(2):
        share(block(k, 0, 0), 0)
    arrive(norm.at[core, y, x, beside], norm_came.at[0])
    norm_send([(pair, {"cols": across})], 1)

    firsts, seconds = (0, half), (quarter, half + quarter)
    first_ranges, second_ranges = [[(at, quarter) for at in starts] for starts in (firsts, seconds)]
    last = (half - tail, width - tail)

    fast_near(0)
    arrive(other_pair, norm_came.at[1])
    norm_send([(norm.at[core, y, x], {"x": wrap(x + i)}) for i in (1, 2, 3)], 2)
    slow_own(0, -1)
    slow_near(0, 0)
    fast_near(1)
    slow_near(1, 0)
    slow_own(0, 1)
    slow_pass(1, 0, 12, 0, quarter)
    slow_own(1, -1)
    slow_own(1, 1)
    fast_far(0)
    slow_own(0, 2)
    slow_pass(0, 0, 12, 0, quarter)
    slow_near(0, -1)
    fast_far(1)
    slow_own(1, 2)
    slow_near(1, -1)
    arrive(three_lines, norm_came.at[2])
    norm_send([(norm.at[core, y], {"y": wrap(y + i)}) for i in (1, 2, 3)], 3)
    for k in range(2):
        slow_pass(k, -1, 12)
    for k in range(2):
        slow_near(k, 1)
        slow_pass(k, 1, 14)
    theirs(0, 8)

    @pl.when(core == 1)
    def _():
        for k in range(2):
            slow_pass(k, 0, 13, quarter, quarter)
            slow_pass(k, 0, 13, quarter, quarter, sibling)

    turn([(0, 0), (-1, 0), (1, 0), (2, 0)])
    slow_near(0, 2)
    slow_pass(0, 2, 15, 0, half - tail)
    slow_pass(0, 2, 17, half - tail, tail)
    turn([(0, -1), (0, 1)])
    slow_near(1, 2)
    slow_pass(1, 2, 16, 0, half - tail)
    slow_pass(1, 2, 18, half - tail, tail)
    turn([(-1, -1), (-1, 1)])
    theirs(1, 2)
    slow_far(12, 3, half, [(-1, (0,), width, core), (0, firsts, quarter, core)], 3)
    turn([(1, -1), (1, 1)])
    arrive(three_planes, norm_came.at[3])
    norm_send([(norm.at[core], {"core": sibling})], 4)

    theirs(2, 2)
    turn([(2, -1), (2, 1)])
    slow_far(14, 1, width, [(1, (0,), width, core)], 4)

    @pl.when(core == 1)
    def _():
        slow_far(13, 1, width, [(0, seconds, quarter, core), (0, seconds, quarter, sibling)], 6)

    theirs(3, 3, half)
    turn([(-1, 2)])
    turn([(0, 2)], first_ranges)
    arrive(norm.at[sibling], norm_came.at[4])
    whole_gain[...] = jnp.sum(norm[...], axis=(0, 3)).reshape(CHIPS, LANES).astype(jnp.bfloat16)
    for k in range(2):
        last_far(k, 15, firsts, half - tail, 5)
    theirs(4, 1)
    turn([(1, 2)])
    for k in range(2):
        last_far(k, 17, last, tail, 7)

    @pl.when(core == 0)
    def _():
        theirs(6, 1)

    turn([(0, 2)], second_ranges)
    theirs(5, 1, width - 2 * tail)
    turn([(2, 2)], [(at, half - tail) for at in firsts])

    @pl.when(core == 1)
    def _():
        arrive(land.at[:, core, pl.ds(0, 3), :, pl.ds(0, half)], sent.at[1])
        arrive(land.at[:, core, pl.ds(0, 3), :, pl.ds(0, half)], gave.at[1])

    @pl.when(core == 0)
    def _():
        arrive(land.at[:, core, pl.ds(0, 1), :, pl.ds(0, half)], sent.at[1])
        arrive(land.at[:, core, pl.ds(0, 1), :, pl.ds(0, half)], gave.at[1])

    theirs(7, 1, 2 * tail)
    turn([(2, 2)], [(at, tail) for at in last])
    arrive(land.at[:, core, pl.ds(0, 14)], sent.at[0])
    arrive(land.at[:, core, pl.ds(0, 15)], gave.at[0])
    for slot, piece in enumerate((one, pair, three_lines, three_planes, norm.at[core])):
        arrive(piece, loaded.at[slot])


def gather(train_gate, low_gate, high_gate, train_up, low_up, high_up, norm_train, norm_step):
    rows, width = train_gate.shape
    rank = low_gate.shape[1]
    vmem = pl.BlockSpec(memory_space=pltpu.VMEM)
    hbm = pl.BlockSpec(memory_space=pltpu.HBM)
    dma = pltpu.SemaphoreType.DMA
    return pl.pallas_call(
        gather_kernel,
        name="gather",
        out_shape=(
            pltpu.VMEM((2, width, 2 * CHIPS * rows), jnp.bfloat16),
            pltpu.VMEM((CHIPS, LANES), jnp.bfloat16),
        ),
        in_specs=[hbm] * 8,
        out_specs=(vmem, vmem),
        scratch_shapes=[
            pltpu.VMEM((2, rows, width), jnp.bfloat16),
            pltpu.VMEM((2, rank, rows), jnp.bfloat16),
            pltpu.VMEM((2, rank, width), jnp.bfloat16),
            pltpu.SMEM((2, 16), jnp.float32),
            pltpu.VMEM((2, SIDE, SIDE, SIDE, 1, LANES), jnp.float32),
            pltpu.VMEM((2, 2, CHIPS, rows, width), jnp.bfloat16),
            dma((8,)), dma((2,)), dma((19,)), dma((2,)), dma((8,)), dma((5,)),
        ],
        compiler_params=pltpu.CompilerParams(
            collective_id=0, has_side_effects=True, vmem_limit_bytes=28 * 2**20
        ),
    )(*(
        pltpu.with_memory_space_constraint(a, pltpu.HBM)
        for a in (train_gate, low_gate.T, high_gate, train_up, low_up.T, high_up, norm_train, norm_step)
    ))


def finish_kernel(turned, gain, serve_gate, serve_up, serve_norm, sems):
    rows = serve_gate.shape[0] // 2
    halves = [pl.ds(i * rows, rows) for i in range(2)]
    pairs = [(turned.at[k, h], out.at[h]) for k, out in enumerate((serve_gate, serve_up)) for h in halves]
    pairs.append((gain, serve_norm))
    copies = [pltpu.make_async_copy(src, dst, sems.at[k]) for k, (src, dst) in enumerate(pairs)]
    for copy in copies:
        copy.start()
    for copy in copies:
        copy.wait()


def finish(turned, gain):
    vmem = pl.BlockSpec(memory_space=pltpu.VMEM)
    hbm = pl.BlockSpec(memory_space=pl.ANY)
    return pl.pallas_call(
        finish_kernel,
        name="finish",
        out_shape=(
            jax.ShapeDtypeStruct(turned.shape[1:], jnp.bfloat16),
            jax.ShapeDtypeStruct(turned.shape[1:], jnp.bfloat16),
            jax.ShapeDtypeStruct(gain.shape, jnp.bfloat16),
        ),
        in_specs=[vmem] * 2,
        out_specs=(hbm, hbm, hbm),
        scratch_shapes=[pltpu.SemaphoreType.DMA((5,))],
        compiler_params=pltpu.CompilerParams(vmem_limit_bytes=4 * 2**20),
    )(turned, gain)


def local(*args):
    serve_gate, serve_up, serve_norm = finish(*gather(*args))
    return serve_gate, serve_up, serve_norm.reshape(-1)


def solution(mesh):
    finer = Mesh(
        mesh.devices.reshape(mesh.shape["trial"], SIDE, SIDE, 2, mesh.shape["cols"]),
        ("trial", "y", "x", "core", "cols"),
    )
    in_specs = (
        P(TRIAL_SHARD, "cols"),
        P(TRIAL_SHARD, None),
        P("trial", "cols"),
        P(TRIAL_SHARD, "cols"),
        P(TRIAL_SHARD, None),
        P("trial", "cols"),
        P(TRIAL_SHARD_COLS),
        P(TRIAL_SHARD_COLS),
    )
    out_specs = (P(("trial", "cols"), None), P(("trial", "cols"), None), P("trial"))
    return jax.shard_map(local, mesh=finer, in_specs=in_specs, out_specs=out_specs, check_vma=False)
```

```python
import functools

import jax
import jax.numpy as jnp
from jax import lax
from jax.experimental import pallas as pl
from jax.experimental.pallas import tpu as pltpu
from jax.sharding import Mesh
from jax.sharding import PartitionSpec as P

TRIAL_SHARD = ("trial", "y", "x", "core")
TRIAL_SHARD_COLS = ("trial", "y", "x", "core", "cols")
MESH_ID = pl.DeviceIdType.MESH
MIX_RATE = 2.0
SIDE = 4
CHIPS = SIDE * SIDE
LANES = 128


def gather_kernel(
    train_gate, low_gate, high_gate, train_up, low_up, high_up, norm_train, norm_step,
    turned, whole_gain,
    train, low, high, gain, rows, norm, land, loaded, sent, came, gave, took, norm_came,
):
    y, x, core, col = (lax.axis_index(a) for a in ("y", "x", "core", "cols"))
    sibling = 1 - core
    width = train.shape[2]
    half, quarter, tail = width // 2, width // 4, width // 8

    def wrap(i):
        return lax.rem(i + SIDE, SIDE)

    pairs = [
        (train_gate, train.at[0]), (high_gate, high.at[0]), (low_gate, low.at[0]),
        (train_up, train.at[1]), (high_up, high.at[1]), (low_up, low.at[1]),
        (norm_train, gain.at[0]), (norm_step, gain.at[1]),
    ]
    loads = [pltpu.make_async_copy(src, dst, loaded.at[k]) for k, (src, dst) in enumerate(pairs)]
    for load in loads[:3]:
        load.start()

    beside, across = col + 1 - 2 * lax.rem(col, 2), wrap(col + 2)
    barrier = pltpu.get_barrier_semaphore()
    partners = [{"cols": across}, {"x": wrap(x + 1)}, {"x": wrap(x - 1)}, {"y": wrap(y + 1)}, {"y": wrap(y - 1)}]
    partners += [{"cols": beside}, {"core": sibling}]
    for device in partners:
        pl.semaphore_signal(barrier, inc=1, device_id=device, device_id_type=MESH_ID)
    for load in loads[3:]:
        load.start()

    def send(piece, sent_sem, came_sem, device):
        pltpu.make_async_remote_copy(
            src_ref=piece, dst_ref=piece, send_sem=sent_sem, recv_sem=came_sem, device_id=device, device_id_type=MESH_ID
        ).start()

    def arrive(piece, sem):
        pltpu.make_async_copy(piece, piece, sem).wait()

    def merge(k, at, size):
        product = lax.dot_general(
            low[k], high[k, :, pl.ds(at, size)], (((0,), (0,)), ((), ())), preferred_element_type=jnp.float32
        )
        merged = train[k, :, pl.ds(at, size)].astype(jnp.float32) + MIX_RATE * product
        land[k, core, y * SIDE + x, :, pl.ds(at, size)] = merged.astype(jnp.bfloat16)

    def place(k, f, s):
        at_x, at_y = (x + f, y + s) if k == 0 else (x + s, y + f)
        return wrap(at_y) * SIDE + wrap(at_x)

    def block(k, f, s, at=0, size=width, side=core):
        return land.at[k, side, place(k, f, s), :, pl.ds(at, size)]

    def push(k, along_fast, step, piece, slot, kind=0):
        axis, at = ("x", x) if along_fast == (k == 0) else ("y", y)
        send(piece, sent.at[kind], came.at[slot], {axis: wrap(at + step)})

    def share(piece, group, kind=0):
        send(piece, gave.at[kind], took.at[group], {"core": sibling})

    def own(k, at=0, size=width):
        for along_fast, slot in ((True, 6 * k), (False, 6 * k + 2)):
            for step in (1, -1):
                push(k, along_fast, step, block(k, 0, 0, at, size), slot)

    def fast_near(k):
        arrive(land.at[k, core, pl.ds(0, 2)], came.at[6 * k])
        push(k, True, 1, block(k, -1, 0, 0, half), 6 * k + 1)
        push(k, True, -1, block(k, 1, 0, half, half), 6 * k + 1)
        for f in (-1, 1):
            share(block(k, f, 0), 0)

    def fast_far(k):
        arrive(land.at[k, core, 0], came.at[6 * k + 1])
        share(block(k, 2, 0), 0)

    def slow_own(k, f):
        for step in (1, -1):
            push(k, False, step, block(k, f, 0), 6 * k + 2 + f % SIDE)

    def slow_near(k, f):
        arrive(land.at[k, core, pl.ds(0, 2)], came.at[6 * k + 2 + f % SIDE])
        for s in (-1, 1):
            share(block(k, f, s), {0: 0, -1: 0, 1: 1, 2: 2}[f])

    def slow_pass(k, f, slot, at=0, size=half, side=core):
        for step, start in ((1, at), (-1, half + at)):
            push(k, False, step, block(k, f, -step, start, size, side), slot, int(f == 0))

    def slow_far(slot, count, size, pieces, group, kind=0):
        arrive(land.at[:, core, pl.ds(0, count), :, pl.ds(0, size)], came.at[slot])
        for k in range(2):
            for f, starts, length, side in pieces:
                for start in starts:
                    share(block(k, f, 2, start, length, side), group, int(f == 0))

    def last_far(k, slot, starts, size, group):
        arrive(land.at[k, core, 0, :, pl.ds(0, 2 * size)], came.at[slot + k])
        for start in starts:
            share(block(k, 2, 2, start, size), group)

    def theirs(group, blocks, size=width):
        arrive(land.at[:, sibling, pl.ds(0, blocks), :, pl.ds(0, size)], took.at[group])

    def turn(chips, ranges=((0, width),)):
        for k in range(2):
            for f, s in chips:
                chip = place(k, f, s)
                lanes = pl.ds(pl.multiple_of(chip * LANES, LANES), LANES)
                for at, size in ranges:
                    tile = [land[k, c, chip, :, pl.ds(at, size)] for c in range(2)]
                    turned[k, pl.ds(at, size), lanes] = jnp.concatenate(tile, axis=0).T

    def norm_send(pieces, slot):
        for piece, device in pieces:
            send(piece, loaded.at[slot], norm_came.at[slot], device)

    one = rows.at[col]
    pair = rows.at[pl.ds(col - lax.rem(col, 2), 2)]
    other_pair = rows.at[pl.ds(across - lax.rem(across, 2), 2)]
    three_lines, three_planes = norm.at[core, y, pl.ds(0, 3)], norm.at[core, pl.ds(0, 3)]

    for load in loads[:3]:
        load.wait()
    merge(0, 0, half)
    pl.semaphore_wait(barrier, len(partners))
    own(0, 0, half)
    merge(0, half, half)
    own(0, half, half)

    for load in loads[3:]:
        load.wait()
    lane = lax.broadcasted_iota(jnp.int32, (1, LANES), 1)
    row = jnp.zeros((1, LANES), jnp.float32)
    first = core * 64 + col * 16
    for i in range(16):
        row = jnp.where(lane == first + i, gain[0, i] + gain[1, i], row)
    rows[col] = row
    merge(1, 0, width)
    norm_send([(one, {"cols": beside})], 0)
    own(1)
    for k in range(2):
        share(block(k, 0, 0), 0)
    arrive(rows.at[beside], norm_came.at[0])
    norm_send([(pair, {"cols": across})], 1)

    firsts, seconds = (0, half), (quarter, half + quarter)
    first_ranges, second_ranges = [[(at, quarter) for at in starts] for starts in (firsts, seconds)]
    last = (half - tail, width - tail)

    fast_near(0)
    arrive(other_pair, norm_came.at[1])
    norm[core, y, x] = jnp.sum(rows[...], axis=0)
    slow_own(0, -1)
    norm_send([(norm.at[core, y, x], {"x": wrap(x + i)}) for i in (1, 2, 3)], 2)
    slow_near(0, 0)
    fast_near(1)
    slow_near(1, 0)
    slow_own(0, 1)
    slow_pass(1, 0, 12, 0, quarter)
    slow_own(1, -1)
    slow_own(1, 1)
    fast_far(0)
    slow_own(0, 2)
    slow_pass(0, 0, 12, 0, quarter)
    slow_near(0, -1)
    fast_far(1)
    slow_own(1, 2)
    slow_near(1, -1)
    arrive(three_lines, norm_came.at[2])
    norm_send([(norm.at[core, y], {"y": wrap(y + i)}) for i in (1, 2, 3)], 3)
    for k in range(2):
        slow_pass(k, -1, 12)
    for k in range(2):
        slow_near(k, 1)
        slow_pass(k, 1, 14)
    theirs(0, 8)

    @pl.when(core == 1)
    def _():
        for k in range(2):
            slow_pass(k, 0, 13, quarter, quarter)
            slow_pass(k, 0, 13, quarter, quarter, sibling)

    turn([(0, 0), (-1, 0), (1, 0), (2, 0)])
    slow_near(0, 2)
    slow_pass(0, 2, 15, 0, half - tail)
    slow_pass(0, 2, 17, half - tail, tail)
    turn([(0, -1), (0, 1)])
    slow_near(1, 2)
    slow_pass(1, 2, 16, 0, half - tail)
    slow_pass(1, 2, 18, half - tail, tail)
    turn([(-1, -1), (-1, 1)])
    theirs(1, 2)
    slow_far(12, 3, half, [(-1, (0,), width, core), (0, firsts, quarter, core)], 3)
    turn([(1, -1), (1, 1)])
    arrive(three_planes, norm_came.at[3])
    norm_send([(norm.at[core], {"core": sibling})], 4)

    theirs(2, 2)
    turn([(2, -1), (2, 1)])
    slow_far(14, 1, width, [(1, (0,), width, core)], 4)

    @pl.when(core == 1)
    def _():
        slow_far(13, 1, width, [(0, seconds, quarter, core), (0, seconds, quarter, sibling)], 6)

    theirs(3, 3, half)
    turn([(-1, 2)])
    turn([(0, 2)], first_ranges)
    arrive(norm.at[sibling], norm_came.at[4])
    whole_gain[...] = jnp.sum(norm[...], axis=0).reshape(CHIPS, LANES).astype(jnp.bfloat16)
    for k in range(2):
        last_far(k, 15, firsts, half - tail, 5)
    theirs(4, 1)
    turn([(1, 2)])
    for k in range(2):
        last_far(k, 17, last, tail, 7)

    @pl.when(core == 0)
    def _():
        theirs(6, 1)

    turn([(0, 2)], second_ranges)
    theirs(5, 1, width - 2 * tail)
    turn([(2, 2)], [(at, half - tail) for at in firsts])

    @pl.when(core == 1)
    def _():
        arrive(land.at[:, core, pl.ds(0, 3), :, pl.ds(0, half)], sent.at[1])
        arrive(land.at[:, core, pl.ds(0, 3), :, pl.ds(0, half)], gave.at[1])

    @pl.when(core == 0)
    def _():
        arrive(land.at[:, core, pl.ds(0, 1), :, pl.ds(0, half)], sent.at[1])
        arrive(land.at[:, core, pl.ds(0, 1), :, pl.ds(0, half)], gave.at[1])

    theirs(7, 1, 2 * tail)
    turn([(2, 2)], [(at, tail) for at in last])
    arrive(land.at[:, core, pl.ds(0, 14)], sent.at[0])
    arrive(land.at[:, core, pl.ds(0, 15)], gave.at[0])
    for slot, piece in enumerate((one, pair, three_lines, three_planes, norm.at[core])):
        arrive(piece, loaded.at[slot])


def gather(train_gate, low_gate, high_gate, train_up, low_up, high_up, norm_train, norm_step):
    rows, width = train_gate.shape
    rank = low_gate.shape[1]
    vmem = pl.BlockSpec(memory_space=pltpu.VMEM)
    hbm = pl.BlockSpec(memory_space=pltpu.HBM)
    dma = pltpu.SemaphoreType.DMA
    return pl.pallas_call(
        gather_kernel,
        name="gather",
        out_shape=(
            pltpu.VMEM((2, width, 2 * CHIPS * rows), jnp.bfloat16),
            pltpu.VMEM((CHIPS, LANES), jnp.bfloat16),
        ),
        in_specs=[hbm] * 8,
        out_specs=(vmem, vmem),
        scratch_shapes=[
            pltpu.VMEM((2, rows, width), jnp.bfloat16),
            pltpu.VMEM((2, rank, rows), jnp.bfloat16),
            pltpu.VMEM((2, rank, width), jnp.bfloat16),
            pltpu.SMEM((2, 16), jnp.float32),
            pltpu.VMEM((SIDE, 1, LANES), jnp.float32),
            pltpu.VMEM((2, SIDE, SIDE, 1, LANES), jnp.float32),
            pltpu.VMEM((2, 2, CHIPS, rows, width), jnp.bfloat16),
            dma((8,)), dma((2,)), dma((19,)), dma((2,)), dma((8,)), dma((5,)),
        ],
        compiler_params=pltpu.CompilerParams(
            collective_id=0, has_side_effects=True, vmem_limit_bytes=28 * 2**20
        ),
    )(*(
        pltpu.with_memory_space_constraint(a, pltpu.HBM)
        for a in (train_gate, low_gate.T, high_gate, train_up, low_up.T, high_up, norm_train, norm_step)
    ))


def finish_kernel(turned, gain, serve_gate, serve_up, serve_norm, sems):
    rows = serve_gate.shape[0] // 2
    halves = [pl.ds(i * rows, rows) for i in range(2)]
    pairs = [(turned.at[k, h], out.at[h]) for k, out in enumerate((serve_gate, serve_up)) for h in halves]
    pairs.append((gain, serve_norm))
    copies = [pltpu.make_async_copy(src, dst, sems.at[k]) for k, (src, dst) in enumerate(pairs)]
    for copy in copies:
        copy.start()
    for copy in copies:
        copy.wait()


def finish(turned, gain):
    vmem = pl.BlockSpec(memory_space=pltpu.VMEM)
    hbm = pl.BlockSpec(memory_space=pl.ANY)
    return pl.pallas_call(
        finish_kernel,
        name="finish",
        out_shape=(
            jax.ShapeDtypeStruct(turned.shape[1:], jnp.bfloat16),
            jax.ShapeDtypeStruct(turned.shape[1:], jnp.bfloat16),
            jax.ShapeDtypeStruct(gain.shape, jnp.bfloat16),
        ),
        in_specs=[vmem] * 2,
        out_specs=(hbm, hbm, hbm),
        scratch_shapes=[pltpu.SemaphoreType.DMA((5,))],
        compiler_params=pltpu.CompilerParams(vmem_limit_bytes=4 * 2**20),
    )(turned, gain)


def local(*args):
    serve_gate, serve_up, serve_norm = finish(*gather(*args))
    return serve_gate, serve_up, serve_norm.reshape(-1)


def solution(mesh):
    finer = Mesh(
        mesh.devices.reshape(mesh.shape["trial"], SIDE, SIDE, 2, mesh.shape["cols"]),
        ("trial", "y", "x", "core", "cols"),
    )
    in_specs = (
        P(TRIAL_SHARD, "cols"),
        P(TRIAL_SHARD, None),
        P("trial", "cols"),
        P(TRIAL_SHARD, "cols"),
        P(TRIAL_SHARD, None),
        P("trial", "cols"),
        P(TRIAL_SHARD_COLS),
        P(TRIAL_SHARD_COLS),
    )
    out_specs = (P(("trial", "cols"), None), P(("trial", "cols"), None), P("trial"))
    return jax.shard_map(local, mesh=finer, in_specs=in_specs, out_specs=out_specs, check_vma=False)
```

```python
import functools

import jax
import jax.numpy as jnp
from jax import lax
from jax.experimental import pallas as pl
from jax.experimental.pallas import tpu as pltpu
from jax.sharding import Mesh
from jax.sharding import PartitionSpec as P

TRIAL_SHARD = ("trial", "y", "x", "core")
TRIAL_SHARD_COLS = ("trial", "y", "x", "core", "cols")
MESH_ID = pl.DeviceIdType.MESH
MIX_RATE = 2.0
SIDE = 4
CHIPS = SIDE * SIDE
LANES = 128


def gather_kernel(
    train_gate, low_gate, high_gate, train_up, low_up, high_up, norm_train, norm_step,
    turned, whole_gain,
    train, low, high, gain, rows, norm, land, loaded, sent, came, gave, took, norm_came,
):
    y, x, core, col = (lax.axis_index(a) for a in ("y", "x", "core", "cols"))
    sibling = 1 - core
    width = train.shape[2]
    half, quarter, tail = width // 2, width // 4, width // 8

    def wrap(i):
        return lax.rem(i + SIDE, SIDE)

    pairs = [
        (train_gate, train.at[0]), (high_gate, high.at[0]), (low_gate, low.at[0]),
        (train_up, train.at[1]), (high_up, high.at[1]), (low_up, low.at[1]),
        (norm_train, gain.at[0]), (norm_step, gain.at[1]),
    ]
    slots = (0, 1, 2, 0, 1, 2, 3, 4)
    loads = [pltpu.make_async_copy(src, dst, loaded.at[slot]) for slot, (src, dst) in zip(slots, pairs)]
    beside, across = col + 1 - 2 * lax.rem(col, 2), wrap(col + 2)
    barrier = pltpu.get_barrier_semaphore()
    partners = [{"cols": across}, {"x": wrap(x + 1)}, {"x": wrap(x - 1)}, {"y": wrap(y + 1)}, {"y": wrap(y - 1)}]
    partners += [{"cols": beside}, {"core": sibling}]
    for device in partners[:5]:
        pl.semaphore_signal(barrier, inc=1, device_id=device, device_id_type=MESH_ID)
    for load in loads[:3]:
        load.start()
    for device in partners[5:]:
        pl.semaphore_signal(barrier, inc=1, device_id=device, device_id_type=MESH_ID)
    for load in loads[6:]:
        load.start()

    def send(piece, sent_sem, came_sem, device):
        pltpu.make_async_remote_copy(
            src_ref=piece, dst_ref=piece, send_sem=sent_sem, recv_sem=came_sem, device_id=device, device_id_type=MESH_ID
        ).start()

    def arrive(piece, sem):
        pltpu.make_async_copy(piece, piece, sem).wait()

    def merge(k, at, size):
        product = lax.dot_general(
            low[k], high[k, :, pl.ds(at, size)], (((0,), (0,)), ((), ())), preferred_element_type=jnp.float32
        )
        merged = train[k, :, pl.ds(at, size)].astype(jnp.float32) + MIX_RATE * product
        land[k, core, y * SIDE + x, :, pl.ds(at, size)] = merged.astype(jnp.bfloat16)

    def place(k, f, s):
        at_x, at_y = (x + f, y + s) if k == 0 else (x + s, y + f)
        return wrap(at_y) * SIDE + wrap(at_x)

    def block(k, f, s, at=0, size=width, side=core):
        return land.at[k, side, place(k, f, s), :, pl.ds(at, size)]

    def push(k, along_fast, step, piece, slot, kind=0):
        axis, at = ("x", x) if along_fast == (k == 0) else ("y", y)
        send(piece, sent.at[kind], came.at[slot], {axis: wrap(at + step)})

    def share(piece, group, kind=0):
        send(piece, gave.at[kind], took.at[group], {"core": sibling})

    def own(k, at=0, size=width):
        for along_fast, slot in ((True, 6 * k), (False, 6 * k + 2)):
            for step in (1, -1):
                push(k, along_fast, step, block(k, 0, 0, at, size), slot)

    def fast_near(k):
        arrive(land.at[k, core, pl.ds(0, 2)], came.at[6 * k])
        push(k, True, 1, block(k, -1, 0, 0, half), 6 * k + 1)
        push(k, True, -1, block(k, 1, 0, half, half), 6 * k + 1)
        for f in (-1, 1):
            share(block(k, f, 0), 0)

    def fast_far(k):
        arrive(land.at[k, core, 0], came.at[6 * k + 1])
        share(block(k, 2, 0), 0)

    def slow_own(k, f):
        for step in (1, -1):
            push(k, False, step, block(k, f, 0), 6 * k + 2 + f % SIDE)

    def slow_near(k, f):
        arrive(land.at[k, core, pl.ds(0, 2)], came.at[6 * k + 2 + f % SIDE])
        for s in (-1, 1):
            share(block(k, f, s), {0: 0, -1: 0, 1: 1, 2: 2}[f])

    def slow_pass(k, f, slot, at=0, size=half, side=core):
        for step, start in ((1, at), (-1, half + at)):
            push(k, False, step, block(k, f, -step, start, size, side), slot, int(f == 0))

    def slow_far(slot, count, size, pieces, group, kind=0):
        arrive(land.at[:, core, pl.ds(0, count), :, pl.ds(0, size)], came.at[slot])
        for k in range(2):
            for f, starts, length, side in pieces:
                for start in starts:
                    share(block(k, f, 2, start, length, side), group, int(f == 0))

    def last_far(k, slot, starts, size, group):
        arrive(land.at[k, core, 0, :, pl.ds(0, 2 * size)], came.at[slot + k])
        for start in starts:
            share(block(k, 2, 2, start, size), group)

    def theirs(group, blocks, size=width):
        arrive(land.at[:, sibling, pl.ds(0, blocks), :, pl.ds(0, size)], took.at[group])

    def turn(chips, ranges=((0, width),)):
        for k in range(2):
            for f, s in chips:
                chip = place(k, f, s)
                lanes = pl.ds(pl.multiple_of(chip * LANES, LANES), LANES)
                for at, size in ranges:
                    tile = [land[k, c, chip, :, pl.ds(at, size)] for c in range(2)]
                    turned[k, pl.ds(at, size), lanes] = jnp.concatenate(tile, axis=0).T

    def norm_send(pieces, slot):
        for piece, device in pieces:
            send(piece, loaded.at[slot], norm_came.at[slot], device)

    one = rows.at[col]
    pair = rows.at[pl.ds(col - lax.rem(col, 2), 2)]
    other_pair = rows.at[pl.ds(across - lax.rem(across, 2), 2)]
    three_lines, three_planes = norm.at[core, y, pl.ds(0, 3)], norm.at[core, pl.ds(0, 3)]

    for load in loads[:3]:
        load.wait()
    merge(0, 0, quarter)
    pl.semaphore_wait(barrier, len(partners))
    own(0, 0, quarter)
    for load in loads[3:6]:
        load.start()
    merge(0, quarter, width - quarter)
    own(0, quarter, width - quarter)

    for load in loads[6:]:
        load.wait()
    lane = lax.broadcasted_iota(jnp.int32, (1, LANES), 1)
    row = jnp.zeros((1, LANES), jnp.float32)
    first = core * 64 + col * 16
    for i in range(16):
        row = jnp.where(lane == first + i, gain[0, i] + gain[1, i], row)
    rows[col] = row
    for load in loads[3:6]:
        load.wait()
    merge(1, 0, width)
    norm_send([(one, {"cols": beside})], 0)
    own(1)
    for k in range(2):
        share(block(k, 0, 0), 0)
    arrive(rows.at[beside], norm_came.at[0])
    norm_send([(pair, {"cols": across})], 1)

    firsts, seconds = (0, half), (quarter, half + quarter)
    first_ranges, second_ranges = [[(at, quarter) for at in starts] for starts in (firsts, seconds)]
    last = (half - tail, width - tail)

    fast_near(0)
    arrive(other_pair, norm_came.at[1])
    norm[core, y, x] = jnp.sum(rows[...], axis=0)
    slow_own(0, -1)
    norm_send([(norm.at[core, y, x], {"x": wrap(x + i)}) for i in (1, 2, 3)], 2)
    slow_near(0, 0)
    fast_near(1)
    slow_near(1, 0)
    slow_own(0, 1)
    slow_pass(1, 0, 12, 0, quarter)
    slow_own(1, -1)
    slow_own(1, 1)
    fast_far(0)
    slow_own(0, 2)
    slow_pass(0, 0, 12, 0, quarter)
    slow_near(0, -1)
    fast_far(1)
    slow_own(1, 2)
    slow_near(1, -1)
    arrive(three_lines, norm_came.at[2])
    norm_send([(norm.at[core, y], {"y": wrap(y + i)}) for i in (1, 2, 3)], 3)
    for k in range(2):
        slow_pass(k, -1, 12)
    for k in range(2):
        slow_near(k, 1)
        slow_pass(k, 1, 14)
    theirs(0, 8)

    @pl.when(core == 1)
    def _():
        for k in range(2):
            slow_pass(k, 0, 13, quarter, quarter)
            slow_pass(k, 0, 13, quarter, quarter, sibling)

    turn([(0, 0), (-1, 0), (1, 0), (2, 0)])
    slow_near(0, 2)
    slow_pass(0, 2, 15, 0, half - tail)
    slow_pass(0, 2, 17, half - tail, tail)
    turn([(0, -1), (0, 1)])
    slow_near(1, 2)
    slow_pass(1, 2, 16, 0, half - tail)
    slow_pass(1, 2, 18, half - tail, tail)
    turn([(-1, -1), (-1, 1)])
    theirs(1, 2)
    slow_far(12, 3, half, [(-1, (0,), width, core), (0, firsts, quarter, core)], 3)
    turn([(1, -1), (1, 1)])
    arrive(three_planes, norm_came.at[3])
    norm_send([(norm.at[core], {"core": sibling})], 4)

    theirs(2, 2)
    turn([(2, -1), (2, 1)])
    slow_far(14, 1, width, [(1, (0,), width, core)], 4)

    @pl.when(core == 1)
    def _():
        slow_far(13, 1, width, [(0, seconds, quarter, core), (0, seconds, quarter, sibling)], 6)

    theirs(3, 3, half)
    turn([(-1, 2)])
    turn([(0, 2)], first_ranges)
    arrive(norm.at[sibling], norm_came.at[4])
    whole_gain[...] = jnp.sum(norm[...], axis=0).reshape(CHIPS, LANES).astype(jnp.bfloat16)
    for k in range(2):
        last_far(k, 15, firsts, half - tail, 5)
    theirs(4, 1)
    turn([(1, 2)])
    for k in range(2):
        last_far(k, 17, last, tail, 7)

    @pl.when(core == 0)
    def _():
        theirs(6, 1)

    turn([(0, 2)], second_ranges)
    theirs(5, 1, width - 2 * tail)
    turn([(2, 2)], [(at, half - tail) for at in firsts])

    @pl.when(core == 1)
    def _():
        arrive(land.at[:, core, pl.ds(0, 3), :, pl.ds(0, half)], sent.at[1])
        arrive(land.at[:, core, pl.ds(0, 3), :, pl.ds(0, half)], gave.at[1])

    @pl.when(core == 0)
    def _():
        arrive(land.at[:, core, pl.ds(0, 1), :, pl.ds(0, half)], sent.at[1])
        arrive(land.at[:, core, pl.ds(0, 1), :, pl.ds(0, half)], gave.at[1])

    theirs(7, 1, 2 * tail)
    turn([(2, 2)], [(at, tail) for at in last])
    arrive(land.at[:, core, pl.ds(0, 14)], sent.at[0])
    arrive(land.at[:, core, pl.ds(0, 15)], gave.at[0])
    for slot, piece in enumerate((one, pair, three_lines, three_planes, norm.at[core])):
        arrive(piece, loaded.at[slot])


def gather(train_gate, low_gate, high_gate, train_up, low_up, high_up, norm_train, norm_step):
    rows, width = train_gate.shape
    rank = low_gate.shape[1]
    vmem = pl.BlockSpec(memory_space=pltpu.VMEM)
    hbm = pl.BlockSpec(memory_space=pltpu.HBM)
    dma = pltpu.SemaphoreType.DMA
    return pl.pallas_call(
        gather_kernel,
        name="gather",
        out_shape=(
            pltpu.VMEM((2, width, 2 * CHIPS * rows), jnp.bfloat16),
            pltpu.VMEM((CHIPS, LANES), jnp.bfloat16),
        ),
        in_specs=[hbm] * 8,
        out_specs=(vmem, vmem),
        scratch_shapes=[
            pltpu.VMEM((2, rows, width), jnp.bfloat16),
            pltpu.VMEM((2, rank, rows), jnp.bfloat16),
            pltpu.VMEM((2, rank, width), jnp.bfloat16),
            pltpu.SMEM((2, 16), jnp.float32),
            pltpu.VMEM((SIDE, 1, LANES), jnp.float32),
            pltpu.VMEM((2, SIDE, SIDE, 1, LANES), jnp.float32),
            pltpu.VMEM((2, 2, CHIPS, rows, width), jnp.bfloat16),
            dma((5,)), dma((2,)), dma((19,)), dma((2,)), dma((8,)), dma((5,)),
        ],
        compiler_params=pltpu.CompilerParams(
            collective_id=0, has_side_effects=True, vmem_limit_bytes=28 * 2**20
        ),
    )(*(
        pltpu.with_memory_space_constraint(a, pltpu.HBM)
        for a in (train_gate, low_gate.T, high_gate, train_up, low_up.T, high_up, norm_train, norm_step)
    ))


def finish_kernel(turned, gain, serve_gate, serve_up, serve_norm, sems):
    rows = serve_gate.shape[0] // 2
    halves = [pl.ds(i * rows, rows) for i in range(2)]
    pairs = [(turned.at[k, h], out.at[h]) for k, out in enumerate((serve_gate, serve_up)) for h in halves]
    pairs.append((gain, serve_norm))
    copies = [pltpu.make_async_copy(src, dst, sems.at[k]) for k, (src, dst) in enumerate(pairs)]
    for copy in copies:
        copy.start()
    for copy in copies:
        copy.wait()


def finish(turned, gain):
    vmem = pl.BlockSpec(memory_space=pltpu.VMEM)
    hbm = pl.BlockSpec(memory_space=pl.ANY)
    return pl.pallas_call(
        finish_kernel,
        name="finish",
        out_shape=(
            jax.ShapeDtypeStruct(turned.shape[1:], jnp.bfloat16),
            jax.ShapeDtypeStruct(turned.shape[1:], jnp.bfloat16),
            jax.ShapeDtypeStruct(gain.shape, jnp.bfloat16),
        ),
        in_specs=[vmem] * 2,
        out_specs=(hbm, hbm, hbm),
        scratch_shapes=[pltpu.SemaphoreType.DMA((5,))],
        compiler_params=pltpu.CompilerParams(vmem_limit_bytes=4 * 2**20),
    )(turned, gain)


def local(*args):
    serve_gate, serve_up, serve_norm = finish(*gather(*args))
    return serve_gate, serve_up, serve_norm.reshape(-1)


def solution(mesh):
    finer = Mesh(
        mesh.devices.reshape(mesh.shape["trial"], SIDE, SIDE, 2, mesh.shape["cols"]),
        ("trial", "y", "x", "core", "cols"),
    )
    in_specs = (
        P(TRIAL_SHARD, "cols"),
        P(TRIAL_SHARD, None),
        P("trial", "cols"),
        P(TRIAL_SHARD, "cols"),
        P(TRIAL_SHARD, None),
        P("trial", "cols"),
        P(TRIAL_SHARD_COLS),
        P(TRIAL_SHARD_COLS),
    )
    out_specs = (P(("trial", "cols"), None), P(("trial", "cols"), None), P("trial"))
    return jax.shard_map(local, mesh=finer, in_specs=in_specs, out_specs=out_specs, check_vma=False)
```

```python
import functools

import jax
import jax.numpy as jnp
from jax import lax
from jax.experimental import pallas as pl
from jax.experimental.pallas import tpu as pltpu
from jax.sharding import Mesh
from jax.sharding import PartitionSpec as P

TRIAL_SHARD = ("trial", "y", "x", "core")
TRIAL_SHARD_COLS = ("trial", "y", "x", "core", "cols")
MESH_ID = pl.DeviceIdType.MESH
MIX_RATE = 2.0
SIDE = 4
CHIPS = SIDE * SIDE
LANES = 128


def gather_kernel(
    train_gate, low_gate, high_gate, train_up, low_up, high_up, norm_train, norm_step,
    turned, whole_gain,
    train, low, high, gain, rows, norm, land, loaded, sent, came, gave, took, norm_came,
):
    y, x, core, col = (lax.axis_index(a) for a in ("y", "x", "core", "cols"))
    sibling = 1 - core
    width = train.shape[2]
    half, quarter, tail = width // 2, width // 4, width // 8

    def wrap(i):
        return lax.rem(i + SIDE, SIDE)

    pairs = [
        (train_gate, train.at[0]), (high_gate, high.at[0]), (low_gate, low.at[0]),
        (train_up, train.at[1]), (high_up, high.at[1]), (low_up, low.at[1]),
        (norm_train, gain.at[0]), (norm_step, gain.at[1]),
    ]
    loads = [pltpu.make_async_copy(src, dst, loaded.at[k]) for k, (src, dst) in enumerate(pairs)]
    for load in loads[:3]:
        load.start()

    beside, across = col + 1 - 2 * lax.rem(col, 2), wrap(col + 2)
    barrier = pltpu.get_barrier_semaphore()
    partners = [{"cols": across}, {"x": wrap(x + 1)}, {"x": wrap(x - 1)}, {"y": wrap(y + 1)}, {"y": wrap(y - 1)}]
    partners += [{"cols": beside}, {"core": sibling}]
    for device in partners:
        pl.semaphore_signal(barrier, inc=1, device_id=device, device_id_type=MESH_ID)
    for load in loads[3:]:
        load.start()

    def send(piece, sent_sem, came_sem, device):
        pltpu.make_async_remote_copy(
            src_ref=piece, dst_ref=piece, send_sem=sent_sem, recv_sem=came_sem, device_id=device, device_id_type=MESH_ID
        ).start()

    def arrive(piece, sem):
        pltpu.make_async_copy(piece, piece, sem).wait()

    def merge(k, at, size):
        product = lax.dot_general(
            low[k], high[k, :, pl.ds(at, size)], (((0,), (0,)), ((), ())), preferred_element_type=jnp.float32
        )
        merged = train[k, :, pl.ds(at, size)].astype(jnp.float32) + MIX_RATE * product
        land[k, core, y * SIDE + x, :, pl.ds(at, size)] = merged.astype(jnp.bfloat16)

    def place(k, f, s):
        at_x, at_y = (x + f, y + s) if k == 0 else (x + s, y + f)
        return wrap(at_y) * SIDE + wrap(at_x)

    def block(k, f, s, at=0, size=width, side=core):
        return land.at[k, side, place(k, f, s), :, pl.ds(at, size)]

    def push(k, along_fast, step, piece, slot, kind=0):
        axis, at = ("x", x) if along_fast == (k == 0) else ("y", y)
        send(piece, sent.at[kind], came.at[slot], {axis: wrap(at + step)})

    def share(piece, group, kind=0):
        send(piece, gave.at[kind], took.at[group], {"core": sibling})

    def own(k, at=0, size=width):
        for along_fast, slot in ((True, 6 * k), (False, 6 * k + 2)):
            for step in (1, -1):
                push(k, along_fast, step, block(k, 0, 0, at, size), slot)

    def fast_near(k):
        arrive(land.at[k, core, pl.ds(0, 2)], came.at[6 * k])
        push(k, True, 1, block(k, -1, 0, 0, half), 6 * k + 1)
        push(k, True, -1, block(k, 1, 0, half, half), 6 * k + 1)
        for f in (-1, 1):
            share(block(k, f, 0), 0)

    def fast_far(k):
        arrive(land.at[k, core, 0], came.at[6 * k + 1])
        share(block(k, 2, 0), 0)

    def slow_own(k, f):
        for step in (1, -1):
            push(k, False, step, block(k, f, 0), 6 * k + 2 + f % SIDE)

    def slow_near(k, f):
        arrive(land.at[k, core, pl.ds(0, 2)], came.at[6 * k + 2 + f % SIDE])
        for s in (-1, 1):
            share(block(k, f, s), {0: 0, -1: 0, 1: 1, 2: 2}[f])

    def slow_pass(k, f, slot, at=0, size=half, side=core):
        for step, start in ((1, at), (-1, half + at)):
            push(k, False, step, block(k, f, -step, start, size, side), slot, int(f == 0))

    def slow_far(slot, count, size, pieces, group, kind=0):
        arrive(land.at[:, core, pl.ds(0, count), :, pl.ds(0, size)], came.at[slot])
        for k in range(2):
            for f, starts, length, side in pieces:
                for start in starts:
                    share(block(k, f, 2, start, length, side), group, int(f == 0))

    def last_far(k, slot, starts, size, group):
        arrive(land.at[k, core, 0, :, pl.ds(0, 2 * size)], came.at[slot + k])
        for start in starts:
            share(block(k, 2, 2, start, size), group)

    def theirs(group, blocks, size=width):
        arrive(land.at[:, sibling, pl.ds(0, blocks), :, pl.ds(0, size)], took.at[group])

    def turn(chips, ranges=((0, width),)):
        def one_array(k, carry):
            for f, s in chips:
                chip = wrap(y + s + k * (f - s)) * SIDE + wrap(x + f + k * (s - f))
                lanes = pl.ds(pl.multiple_of(chip * LANES, LANES), LANES)
                for at, size in ranges:
                    tile = [land[k, c, chip, :, pl.ds(at, size)] for c in range(2)]
                    turned[k, pl.ds(at, size), lanes] = jnp.concatenate(tile, axis=0).T
            return carry

        lax.fori_loop(0, 2, one_array, 0)

    def norm_send(pieces, slot):
        for piece, device in pieces:
            send(piece, loaded.at[slot], norm_came.at[slot], device)

    one = rows.at[col]
    pair = rows.at[pl.ds(col - lax.rem(col, 2), 2)]
    other_pair = rows.at[pl.ds(across - lax.rem(across, 2), 2)]
    three_lines, three_planes = norm.at[core, y, pl.ds(0, 3)], norm.at[core, pl.ds(0, 3)]

    for load in loads[:3]:
        load.wait()
    merge(0, 0, half)
    pl.semaphore_wait(barrier, len(partners))
    own(0, 0, half)
    merge(0, half, half)
    own(0, half, half)

    for load in loads[3:]:
        load.wait()
    lane = lax.broadcasted_iota(jnp.int32, (1, LANES), 1)
    row = jnp.zeros((1, LANES), jnp.float32)
    first = core * 64 + col * 16
    for i in range(16):
        row = jnp.where(lane == first + i, gain[0, i] + gain[1, i], row)
    rows[col] = row
    merge(1, 0, width)
    norm_send([(one, {"cols": beside})], 0)
    own(1)
    for k in range(2):
        share(block(k, 0, 0), 0)
    arrive(rows.at[beside], norm_came.at[0])
    norm_send([(pair, {"cols": across})], 1)

    firsts, seconds = (0, half), (quarter, half + quarter)
    first_ranges, second_ranges = [[(at, quarter) for at in starts] for starts in (firsts, seconds)]
    last = (half - tail, width - tail)

    fast_near(0)
    arrive(other_pair, norm_came.at[1])
    norm[core, y, x] = jnp.sum(rows[...], axis=0)
    slow_own(0, -1)
    norm_send([(norm.at[core, y, x], {"x": wrap(x + i)}) for i in (1, 2, 3)], 2)
    slow_near(0, 0)
    fast_near(1)
    slow_near(1, 0)
    slow_own(0, 1)
    slow_pass(1, 0, 12, 0, quarter)
    slow_own(1, -1)
    slow_own(1, 1)
    fast_far(0)
    slow_own(0, 2)
    slow_pass(0, 0, 12, 0, quarter)
    slow_near(0, -1)
    fast_far(1)
    slow_own(1, 2)
    slow_near(1, -1)
    arrive(three_lines, norm_came.at[2])
    norm_send([(norm.at[core, y], {"y": wrap(y + i)}) for i in (1, 2, 3)], 3)
    for k in range(2):
        slow_pass(k, -1, 12)
    for k in range(2):
        slow_near(k, 1)
        slow_pass(k, 1, 14)
    theirs(0, 8)

    @pl.when(core == 1)
    def _():
        for k in range(2):
            slow_pass(k, 0, 13, quarter, quarter)
            slow_pass(k, 0, 13, quarter, quarter, sibling)

    turn([(0, 0), (-1, 0), (1, 0), (2, 0)])
    slow_near(0, 2)
    slow_pass(0, 2, 15, 0, half - tail)
    slow_pass(0, 2, 17, half - tail, tail)
    turn([(0, -1), (0, 1)])
    slow_near(1, 2)
    slow_pass(1, 2, 16, 0, half - tail)
    slow_pass(1, 2, 18, half - tail, tail)
    turn([(-1, -1), (-1, 1)])
    theirs(1, 2)
    slow_far(12, 3, half, [(-1, (0,), width, core), (0, firsts, quarter, core)], 3)
    turn([(1, -1), (1, 1)])
    arrive(three_planes, norm_came.at[3])
    norm_send([(norm.at[core], {"core": sibling})], 4)

    theirs(2, 2)
    turn([(2, -1), (2, 1)])
    slow_far(14, 1, width, [(1, (0,), width, core)], 4)

    @pl.when(core == 1)
    def _():
        slow_far(13, 1, width, [(0, seconds, quarter, core), (0, seconds, quarter, sibling)], 6)

    theirs(3, 3, half)
    turn([(-1, 2)])
    turn([(0, 2)], first_ranges)
    arrive(norm.at[sibling], norm_came.at[4])
    whole_gain[...] = jnp.sum(norm[...], axis=0).reshape(CHIPS, LANES).astype(jnp.bfloat16)
    for k in range(2):
        last_far(k, 15, firsts, half - tail, 5)
    theirs(4, 1)
    turn([(1, 2)])
    for k in range(2):
        last_far(k, 17, last, tail, 7)

    @pl.when(core == 0)
    def _():
        theirs(6, 1)

    turn([(0, 2)], second_ranges)
    theirs(5, 1, width - 2 * tail)
    turn([(2, 2)], [(at, half - tail) for at in firsts])

    @pl.when(core == 1)
    def _():
        arrive(land.at[:, core, pl.ds(0, 3), :, pl.ds(0, half)], sent.at[1])
        arrive(land.at[:, core, pl.ds(0, 3), :, pl.ds(0, half)], gave.at[1])

    @pl.when(core == 0)
    def _():
        arrive(land.at[:, core, pl.ds(0, 1), :, pl.ds(0, half)], sent.at[1])
        arrive(land.at[:, core, pl.ds(0, 1), :, pl.ds(0, half)], gave.at[1])

    theirs(7, 1, 2 * tail)
    turn([(2, 2)], [(at, tail) for at in last])
    arrive(land.at[:, core, pl.ds(0, 14)], sent.at[0])
    arrive(land.at[:, core, pl.ds(0, 15)], gave.at[0])
    for slot, piece in enumerate((one, pair, three_lines, three_planes, norm.at[core])):
        arrive(piece, loaded.at[slot])


def gather(train_gate, low_gate, high_gate, train_up, low_up, high_up, norm_train, norm_step):
    rows, width = train_gate.shape
    rank = low_gate.shape[1]
    vmem = pl.BlockSpec(memory_space=pltpu.VMEM)
    hbm = pl.BlockSpec(memory_space=pltpu.HBM)
    dma = pltpu.SemaphoreType.DMA
    return pl.pallas_call(
        gather_kernel,
        name="gather",
        out_shape=(
            pltpu.VMEM((2, width, 2 * CHIPS * rows), jnp.bfloat16),
            pltpu.VMEM((CHIPS, LANES), jnp.bfloat16),
        ),
        in_specs=[hbm] * 8,
        out_specs=(vmem, vmem),
        scratch_shapes=[
            pltpu.VMEM((2, rows, width), jnp.bfloat16),
            pltpu.VMEM((2, rank, rows), jnp.bfloat16),
            pltpu.VMEM((2, rank, width), jnp.bfloat16),
            pltpu.SMEM((2, 16), jnp.float32),
            pltpu.VMEM((SIDE, 1, LANES), jnp.float32),
            pltpu.VMEM((2, SIDE, SIDE, 1, LANES), jnp.float32),
            pltpu.VMEM((2, 2, CHIPS, rows, width), jnp.bfloat16),
            dma((8,)), dma((2,)), dma((19,)), dma((2,)), dma((8,)), dma((5,)),
        ],
        compiler_params=pltpu.CompilerParams(
            collective_id=0, has_side_effects=True, vmem_limit_bytes=28 * 2**20
        ),
    )(*(
        pltpu.with_memory_space_constraint(a, pltpu.HBM)
        for a in (train_gate, low_gate.T, high_gate, train_up, low_up.T, high_up, norm_train, norm_step)
    ))


def finish_kernel(turned, gain, serve_gate, serve_up, serve_norm, sems):
    rows = serve_gate.shape[0] // 2
    halves = [pl.ds(i * rows, rows) for i in range(2)]
    pairs = [(turned.at[k, h], out.at[h]) for k, out in enumerate((serve_gate, serve_up)) for h in halves]
    pairs.append((gain, serve_norm))
    copies = [pltpu.make_async_copy(src, dst, sems.at[k]) for k, (src, dst) in enumerate(pairs)]
    for copy in copies:
        copy.start()
    for copy in copies:
        copy.wait()


def finish(turned, gain):
    vmem = pl.BlockSpec(memory_space=pltpu.VMEM)
    hbm = pl.BlockSpec(memory_space=pl.ANY)
    return pl.pallas_call(
        finish_kernel,
        name="finish",
        out_shape=(
            jax.ShapeDtypeStruct(turned.shape[1:], jnp.bfloat16),
            jax.ShapeDtypeStruct(turned.shape[1:], jnp.bfloat16),
            jax.ShapeDtypeStruct(gain.shape, jnp.bfloat16),
        ),
        in_specs=[vmem] * 2,
        out_specs=(hbm, hbm, hbm),
        scratch_shapes=[pltpu.SemaphoreType.DMA((5,))],
        compiler_params=pltpu.CompilerParams(vmem_limit_bytes=4 * 2**20),
    )(turned, gain)


def local(*args):
    serve_gate, serve_up, serve_norm = finish(*gather(*args))
    return serve_gate, serve_up, serve_norm.reshape(-1)


def solution(mesh):
    finer = Mesh(
        mesh.devices.reshape(mesh.shape["trial"], SIDE, SIDE, 2, mesh.shape["cols"]),
        ("trial", "y", "x", "core", "cols"),
    )
    in_specs = (
        P(TRIAL_SHARD, "cols"),
        P(TRIAL_SHARD, None),
        P("trial", "cols"),
        P(TRIAL_SHARD, "cols"),
        P(TRIAL_SHARD, None),
        P("trial", "cols"),
        P(TRIAL_SHARD_COLS),
        P(TRIAL_SHARD_COLS),
    )
    out_specs = (P(("trial", "cols"), None), P(("trial", "cols"), None), P("trial"))
    return jax.shard_map(local, mesh=finer, in_specs=in_specs, out_specs=out_specs, check_vma=False)
```

```python
import functools

import jax
import jax.numpy as jnp
from jax import lax
from jax.experimental import pallas as pl
from jax.experimental.pallas import tpu as pltpu
from jax.sharding import Mesh
from jax.sharding import PartitionSpec as P

TRIAL_SHARD = ("trial", "y", "x", "core")
TRIAL_SHARD_COLS = ("trial", "y", "x", "core", "cols")
MESH_ID = pl.DeviceIdType.MESH
MIX_RATE = 2.0
SIDE = 4
CHIPS = SIDE * SIDE
LANES = 128


def gather_kernel(
    train_gate, low_gate, high_gate, train_up, low_up, high_up, norm_train, norm_step,
    turned, whole_gain,
    train, low, high, gain, rows, norm, land, loaded, sent, came, gave, took, norm_came,
):
    y, x, core, col = (lax.axis_index(a) for a in ("y", "x", "core", "cols"))
    sibling = 1 - core
    width = train.shape[2]
    half, quarter, tail = width // 2, width // 4, width // 16

    def wrap(i):
        return lax.rem(i + SIDE, SIDE)

    pairs = [
        (train_gate, train.at[0]), (high_gate, high.at[0]), (low_gate, low.at[0]),
        (train_up, train.at[1]), (high_up, high.at[1]), (low_up, low.at[1]),
        (norm_train, gain.at[0]), (norm_step, gain.at[1]),
    ]
    loads = [pltpu.make_async_copy(src, dst, loaded.at[k]) for k, (src, dst) in enumerate(pairs)]
    for load in loads[:3]:
        load.start()

    beside, across = col + 1 - 2 * lax.rem(col, 2), wrap(col + 2)
    barrier = pltpu.get_barrier_semaphore()
    partners = [{"cols": across}, {"x": wrap(x + 1)}, {"x": wrap(x - 1)}, {"y": wrap(y + 1)}, {"y": wrap(y - 1)}]
    partners += [{"cols": beside}, {"core": sibling}]
    for device in partners:
        pl.semaphore_signal(barrier, inc=1, device_id=device, device_id_type=MESH_ID)
    for load in loads[3:]:
        load.start()

    def send(piece, sent_sem, came_sem, device):
        pltpu.make_async_remote_copy(
            src_ref=piece, dst_ref=piece, send_sem=sent_sem, recv_sem=came_sem, device_id=device, device_id_type=MESH_ID
        ).start()

    def arrive(piece, sem):
        pltpu.make_async_copy(piece, piece, sem).wait()

    def merge(k, at, size):
        product = lax.dot_general(
            low[k], high[k, :, pl.ds(at, size)], (((0,), (0,)), ((), ())), preferred_element_type=jnp.float32
        )
        merged = train[k, :, pl.ds(at, size)].astype(jnp.float32) + MIX_RATE * product
        land[k, core, y * SIDE + x, :, pl.ds(at, size)] = merged.astype(jnp.bfloat16)

    def place(k, f, s):
        at_x, at_y = (x + f, y + s) if k == 0 else (x + s, y + f)
        return wrap(at_y) * SIDE + wrap(at_x)

    def block(k, f, s, at=0, size=width, side=core):
        return land.at[k, side, place(k, f, s), :, pl.ds(at, size)]

    def push(k, along_fast, step, piece, slot, kind=0):
        axis, at = ("x", x) if along_fast == (k == 0) else ("y", y)
        send(piece, sent.at[kind], came.at[slot], {axis: wrap(at + step)})

    def share(piece, group, kind=0):
        send(piece, gave.at[kind], took.at[group], {"core": sibling})

    def own(k, at=0, size=width):
        for along_fast, slot in ((True, 6 * k), (False, 6 * k + 2)):
            for step in (1, -1):
                push(k, along_fast, step, block(k, 0, 0, at, size), slot)

    def fast_near(k):
        arrive(land.at[k, core, pl.ds(0, 2)], came.at[6 * k])
        push(k, True, 1, block(k, -1, 0, 0, half), 6 * k + 1)
        push(k, True, -1, block(k, 1, 0, half, half), 6 * k + 1)
        for f in (-1, 1):
            share(block(k, f, 0), 0)

    def fast_far(k):
        arrive(land.at[k, core, 0], came.at[6 * k + 1])
        share(block(k, 2, 0), 0)

    def slow_own(k, f):
        for step in (1, -1):
            push(k, False, step, block(k, f, 0), 6 * k + 2 + f % SIDE)

    def slow_near(k, f):
        arrive(land.at[k, core, pl.ds(0, 2)], came.at[6 * k + 2 + f % SIDE])
        for s in (-1, 1):
            share(block(k, f, s), {0: 0, -1: 0, 1: 1, 2: 2}[f])

    def slow_pass(k, f, slot, at=0, size=half, side=core):
        for step, start in ((1, at), (-1, half + at)):
            push(k, False, step, block(k, f, -step, start, size, side), slot, int(f == 0))

    def slow_far(slot, count, size, pieces, group, kind=0):
        arrive(land.at[:, core, pl.ds(0, count), :, pl.ds(0, size)], came.at[slot])
        for k in range(2):
            for f, starts, length, side in pieces:
                for start in starts:
                    share(block(k, f, 2, start, length, side), group, int(f == 0))

    def last_far(k, slot, starts, size, group):
        arrive(land.at[k, core, 0, :, pl.ds(0, 2 * size)], came.at[slot + k])
        for start in starts:
            share(block(k, 2, 2, start, size), group)

    def theirs(group, blocks, size=width):
        arrive(land.at[:, sibling, pl.ds(0, blocks), :, pl.ds(0, size)], took.at[group])

    def turn(chips, ranges=((0, width),)):
        for k in range(2):
            for f, s in chips:
                chip = place(k, f, s)
                lanes = pl.ds(pl.multiple_of(chip * LANES, LANES), LANES)
                for at, size in ranges:
                    tile = [land[k, c, chip, :, pl.ds(at, size)] for c in range(2)]
                    turned[k, pl.ds(at, size), lanes] = jnp.concatenate(tile, axis=0).T

    def norm_send(pieces, slot):
        for piece, device in pieces:
            send(piece, loaded.at[slot], norm_came.at[slot], device)

    one = rows.at[col]
    pair = rows.at[pl.ds(col - lax.rem(col, 2), 2)]
    other_pair = rows.at[pl.ds(across - lax.rem(across, 2), 2)]
    three_lines, three_planes = norm.at[core, y, pl.ds(0, 3)], norm.at[core, pl.ds(0, 3)]

    for load in loads[:3]:
        load.wait()
    merge(0, 0, half)
    pl.semaphore_wait(barrier, len(partners))
    own(0, 0, half)
    merge(0, half, half)
    own(0, half, half)

    for load in loads[3:]:
        load.wait()
    lane = lax.broadcasted_iota(jnp.int32, (1, LANES), 1)
    row = jnp.zeros((1, LANES), jnp.float32)
    first = core * 64 + col * 16
    for i in range(16):
        row = jnp.where(lane == first + i, gain[0, i] + gain[1, i], row)
    rows[col] = row
    merge(1, 0, width)
    norm_send([(one, {"cols": beside})], 0)
    own(1)
    for k in range(2):
        share(block(k, 0, 0), 0)
    arrive(rows.at[beside], norm_came.at[0])
    norm_send([(pair, {"cols": across})], 1)

    firsts, seconds = (0, half), (quarter, half + quarter)
    first_ranges, second_ranges = [[(at, quarter) for at in starts] for starts in (firsts, seconds)]
    last = (half - tail, width - tail)

    fast_near(0)
    arrive(other_pair, norm_came.at[1])
    norm[core, y, x] = jnp.sum(rows[...], axis=0)
    slow_own(0, -1)
    norm_send([(norm.at[core, y, x], {"x": wrap(x + i)}) for i in (1, 2, 3)], 2)
    slow_near(0, 0)
    fast_near(1)
    slow_near(1, 0)
    slow_own(0, 1)
    slow_pass(1, 0, 12, 0, quarter)
    slow_own(1, -1)
    slow_own(1, 1)
    fast_far(0)
    slow_own(0, 2)
    slow_pass(0, 0, 12, 0, quarter)
    slow_near(0, -1)
    fast_far(1)
    slow_own(1, 2)
    slow_near(1, -1)
    arrive(three_lines, norm_came.at[2])
    norm_send([(norm.at[core, y], {"y": wrap(y + i)}) for i in (1, 2, 3)], 3)
    for k in range(2):
        slow_pass(k, -1, 12)
    for k in range(2):
        slow_near(k, 1)
        slow_pass(k, 1, 14)
    theirs(0, 8)

    @pl.when(core == 1)
    def _():
        for k in range(2):
            slow_pass(k, 0, 13, quarter, quarter)
            slow_pass(k, 0, 13, quarter, quarter, sibling)

    turn([(0, 0), (-1, 0), (1, 0), (2, 0)])
    slow_near(0, 2)
    slow_pass(0, 2, 15, 0, half - tail)
    slow_pass(0, 2, 17, half - tail, tail)
    turn([(0, -1), (0, 1)])
    slow_near(1, 2)
    slow_pass(1, 2, 16, 0, half - tail)
    slow_pass(1, 2, 18, half - tail, tail)
    turn([(-1, -1), (-1, 1)])
    theirs(1, 2)
    slow_far(12, 3, half, [(-1, (0,), width, core), (0, firsts, quarter, core)], 3)
    turn([(1, -1), (1, 1)])
    arrive(three_planes, norm_came.at[3])
    norm_send([(norm.at[core], {"core": sibling})], 4)

    theirs(2, 2)
    turn([(2, -1), (2, 1)])
    slow_far(14, 1, width, [(1, (0,), width, core)], 4)

    @pl.when(core == 1)
    def _():
        slow_far(13, 1, width, [(0, seconds, quarter, core), (0, seconds, quarter, sibling)], 6)

    theirs(3, 3, half)
    turn([(-1, 2)])
    turn([(0, 2)], first_ranges)
    arrive(norm.at[sibling], norm_came.at[4])
    whole_gain[...] = jnp.sum(norm[...], axis=0).reshape(CHIPS, LANES).astype(jnp.bfloat16)
    for k in range(2):
        last_far(k, 15, firsts, half - tail, 5)
    theirs(4, 1)
    turn([(1, 2)])
    for k in range(2):
        last_far(k, 17, last, tail, 7)

    @pl.when(core == 0)
    def _():
        theirs(6, 1)

    turn([(0, 2)], second_ranges)
    theirs(5, 1, width - 2 * tail)
    turn([(2, 2)], [(at, half - tail) for at in firsts])

    @pl.when(core == 1)
    def _():
        arrive(land.at[:, core, pl.ds(0, 3), :, pl.ds(0, half)], sent.at[1])
        arrive(land.at[:, core, pl.ds(0, 3), :, pl.ds(0, half)], gave.at[1])

    @pl.when(core == 0)
    def _():
        arrive(land.at[:, core, pl.ds(0, 1), :, pl.ds(0, half)], sent.at[1])
        arrive(land.at[:, core, pl.ds(0, 1), :, pl.ds(0, half)], gave.at[1])

    theirs(7, 1, 2 * tail)
    turn([(2, 2)], [(at, tail) for at in last])
    arrive(land.at[:, core, pl.ds(0, 14)], sent.at[0])
    arrive(land.at[:, core, pl.ds(0, 15)], gave.at[0])
    for slot, piece in enumerate((one, pair, three_lines, three_planes, norm.at[core])):
        arrive(piece, loaded.at[slot])


def gather(train_gate, low_gate, high_gate, train_up, low_up, high_up, norm_train, norm_step):
    rows, width = train_gate.shape
    rank = low_gate.shape[1]
    vmem = pl.BlockSpec(memory_space=pltpu.VMEM)
    hbm = pl.BlockSpec(memory_space=pltpu.HBM)
    dma = pltpu.SemaphoreType.DMA
    return pl.pallas_call(
        gather_kernel,
        name="gather",
        out_shape=(
            pltpu.VMEM((2, width, 2 * CHIPS * rows), jnp.bfloat16),
            pltpu.VMEM((CHIPS, LANES), jnp.bfloat16),
        ),
        in_specs=[hbm] * 8,
        out_specs=(vmem, vmem),
        scratch_shapes=[
            pltpu.VMEM((2, rows, width), jnp.bfloat16),
            pltpu.VMEM((2, rank, rows), jnp.bfloat16),
            pltpu.VMEM((2, rank, width), jnp.bfloat16),
            pltpu.SMEM((2, 16), jnp.float32),
            pltpu.VMEM((SIDE, 1, LANES), jnp.float32),
            pltpu.VMEM((2, SIDE, SIDE, 1, LANES), jnp.float32),
            pltpu.VMEM((2, 2, CHIPS, rows, width), jnp.bfloat16),
            dma((8,)), dma((2,)), dma((19,)), dma((2,)), dma((8,)), dma((5,)),
        ],
        compiler_params=pltpu.CompilerParams(
            collective_id=0, has_side_effects=True, vmem_limit_bytes=28 * 2**20
        ),
    )(*(
        pltpu.with_memory_space_constraint(a, pltpu.HBM)
        for a in (train_gate, low_gate.T, high_gate, train_up, low_up.T, high_up, norm_train, norm_step)
    ))


def finish_kernel(turned, gain, serve_gate, serve_up, serve_norm, sems):
    rows = serve_gate.shape[0] // 2
    halves = [pl.ds(i * rows, rows) for i in range(2)]
    pairs = [(turned.at[k, h], out.at[h]) for k, out in enumerate((serve_gate, serve_up)) for h in halves]
    pairs.append((gain, serve_norm))
    copies = [pltpu.make_async_copy(src, dst, sems.at[k]) for k, (src, dst) in enumerate(pairs)]
    for copy in copies:
        copy.start()
    for copy in copies:
        copy.wait()


def finish(turned, gain):
    vmem = pl.BlockSpec(memory_space=pltpu.VMEM)
    hbm = pl.BlockSpec(memory_space=pl.ANY)
    return pl.pallas_call(
        finish_kernel,
        name="finish",
        out_shape=(
            jax.ShapeDtypeStruct(turned.shape[1:], jnp.bfloat16),
            jax.ShapeDtypeStruct(turned.shape[1:], jnp.bfloat16),
            jax.ShapeDtypeStruct(gain.shape, jnp.bfloat16),
        ),
        in_specs=[vmem] * 2,
        out_specs=(hbm, hbm, hbm),
        scratch_shapes=[pltpu.SemaphoreType.DMA((5,))],
        compiler_params=pltpu.CompilerParams(vmem_limit_bytes=4 * 2**20),
    )(turned, gain)


def local(*args):
    serve_gate, serve_up, serve_norm = finish(*gather(*args))
    return serve_gate, serve_up, serve_norm.reshape(-1)


def solution(mesh):
    finer = Mesh(
        mesh.devices.reshape(mesh.shape["trial"], SIDE, SIDE, 2, mesh.shape["cols"]),
        ("trial", "y", "x", "core", "cols"),
    )
    in_specs = (
        P(TRIAL_SHARD, "cols"),
        P(TRIAL_SHARD, None),
        P("trial", "cols"),
        P(TRIAL_SHARD, "cols"),
        P(TRIAL_SHARD, None),
        P("trial", "cols"),
        P(TRIAL_SHARD_COLS),
        P(TRIAL_SHARD_COLS),
    )
    out_specs = (P(("trial", "cols"), None), P(("trial", "cols"), None), P("trial"))
    return jax.shard_map(local, mesh=finer, in_specs=in_specs, out_specs=out_specs, check_vma=False)
```
